256 devices in a mesh: dp: 8 (over z), space: 2 (over core), mp: 16 (over y, x).
Axes of the slice: x: 4, y: 4, z: 8, core: 2. Of those that a mesh axis runs over, the one named last changes fastest.
Arguments:
- features: bfloat16 [128, 64, 1024], P(('dp', 'space'), None, 'mp'), parts along dimension 0, may hold values from -6 to 6
- deconv_weight: bfloat16 [4, 512, 1024], P(None, 'mp'), may hold values from -0.1875 to 0.1875
- deconv_bias: float32 [512], P('mp'), may hold values from -3 to 3
- lateral_eight: bfloat16 [256, 512], P('mp'), may hold values from -0.25 to 0.25
- lateral_coarse: bfloat16 [2, 256, 1024], P(None, 'mp'), may hold values from -0.1875 to 0.1875
- output_conv: bfloat16 [3, 256, 9, 256], P(None, 'mp'), may hold values from -0.125 to 0.125
- norm_gain: float32 [6, 256], replicated, may hold values from 0.1 to 1.9
- norm_shift: float32 [6, 256], replicated, may hold values from -3 to 3
Outputs:
- level_eight: bfloat16 [256, 32768], P('mp', ('dp', 'space')), parts along dimension 1
- level_sixteen: bfloat16 [256, 8192], P('mp', ('dp', 'space')), parts along dimension 1
- level_thirty: bfloat16 [256, 2048], P('mp', ('dp', 'space')), parts along dimension 1
- level_sixty: bfloat16 [256, 512], P('mp', ('dp', 'space')), parts along dimension 1
The draws below stay inside these ranges and needn't reach their ends.
There are 8 independent parts, one for each index of `dp`. The reference program is written for one: setup_inputs(seed, part) draws one part's arguments, and reference() takes and returns one part's arrays. A program takes and returns all parts, laid end to end along the dimension named above; an argument that names none is the same for every part. Nothing has to cross between parts.
All inputs are finite; a program needn't handle non-finite values.
Results may differ from the reference program's by a relative error of at most 0.015.
Values may be sent and summed in bfloat16 or wider, within the bound.
No kernel may reach another device: no remote copies, remote signals or barrier semaphores. Data moves between devices by JAX's collectives and lax.ppermute only.
A program may use at most 64 MiB of HBM per device.

```python
import jax
import jax.numpy as jnp
from jax import lax

D = 1024
NECK = 256
HALF = 512
COLS = 64
GRID = 16


def block_levels(stream_key, extent, split, least, high):
    gain = 1.0
    for axis_at, blocks in split:
        steps = jax.random.uniform(jax.random.fold_in(jax.random.fold_in(stream_key, 6), axis_at), (blocks,), jnp.float32, least / len(split), high / len(split))
        gain = gain * jnp.repeat(jnp.exp(steps), extent[axis_at] // blocks).reshape((-1,) + (1,) * (len(extent) - 1 - axis_at))
    return gain


def gaussian(key, extent, deviation, most, shards=(), held_as=jnp.bfloat16):
    loudness = block_levels(key, extent, shards, -0.22, 0.18) if shards else 1.0
    result = jax.random.normal(key, extent, jnp.float32) * deviation * loudness
    return jnp.minimum(jnp.maximum(result, -most), most).astype(held_as)


def setup_inputs(seed: int = 0, part: int = 0) -> dict:
    splits = jax.random.split(jax.random.key(seed), 9)
    own_keys = jax.random.split(jax.random.fold_in(splits[8], part), 9)
    return {
        "features": gaussian(own_keys[0], (GRID, COLS, D), 1.0, 6.0, ((0, 2), (2, 16))),
        "deconv_weight": gaussian(splits[1], (4, HALF, D), D ** -0.5, 0.1875, ((1, 16),)),
        "deconv_bias": gaussian(splits[2], (HALF,), 0.5, 3.0, ((0, 16),), jnp.float32),
        "lateral_eight": gaussian(splits[3], (NECK, HALF), HALF ** -0.5, 0.25, ((0, 16),)),
        "lateral_coarse": gaussian(splits[4], (2, NECK, D), D ** -0.5, 0.1875, ((1, 16),)),
        "output_conv": gaussian(splits[5], (3, NECK, 9, NECK), (9 * NECK) ** -0.5, 0.125, ((1, 16),)),
        "norm_gain": jnp.clip(1.0 + 0.18 * jax.random.normal(splits[6], (6, NECK), jnp.float32), 0.1, 1.9),
        "norm_shift": gaussian(splits[7], (6, NECK), 0.5, 3.0, (), jnp.float32),
    }


EPSILON = 1e-06

def channel_norm(values, gain_row, shift_row):
    floats = values.astype(jnp.float32)
    center = lax.optimization_barrier(jnp.mean(floats, axis=-1, keepdims=True))
    spread = lax.optimization_barrier(jnp.mean(floats * floats, axis=-1, keepdims=True)) - center * center
    scaled = (floats - center) * lax.rsqrt(spread + EPSILON)
    return (scaled * gain_row + shift_row).astype(jnp.bfloat16)

def conv_three(normed, weight):
    height, width, _ = normed.shape
    padded = jnp.pad(normed, ((1, 1), (1, 1), (0, 0)))
    totals = jnp.zeros((height * width, weight.shape[0]), jnp.float32)
    for tap_index in range(9):
        row_off = tap_index // 3
        col_off = tap_index % 3
        window = padded[row_off:row_off + height, col_off:col_off + width].reshape(height * width, -1)
        totals = totals + jnp.dot(window, weight[:, tap_index, :].T, preferred_element_type=jnp.float32)
    return totals.reshape(height, width, -1).astype(jnp.bfloat16)

def pool_pairs(values):
    height, width, depth = values.shape
    return lax.optimization_barrier(jnp.max(values.reshape(height // 2, 2, width // 2, 2, depth), axis=(1, 3)))

def channel_major(values):
    return values.transpose(2, 0, 1).reshape(values.shape[2], -1)

def reference(features, deconv_weight, deconv_bias, lateral_eight, lateral_coarse, output_conv, norm_gain, norm_shift):
    height, width, depth = features.shape
    half_width = deconv_weight.shape[1]
    flattened = features.reshape(height * width, depth)
    raised = jnp.dot(flattened, deconv_weight.reshape(4 * half_width, depth).T, preferred_element_type=jnp.float32)
    raised = raised.reshape(height, width, 2, 2, half_width) + deconv_bias
    upsampled = raised.transpose(0, 2, 1, 3, 4).reshape(2 * height, 2 * width, half_width).astype(jnp.bfloat16)
    pooled = pool_pairs(features)
    lat_a = jnp.dot(upsampled.reshape(-1, half_width), lateral_eight.T, preferred_element_type=jnp.float32)
    lat_a = lat_a.reshape(2 * height, 2 * width, -1).astype(jnp.bfloat16)
    lat_b = jnp.dot(flattened, lateral_coarse[0].T, preferred_element_type=jnp.float32)
    lat_b = lat_b.reshape(height, width, -1).astype(jnp.bfloat16)
    lat_c = jnp.dot(pooled.reshape(-1, depth), lateral_coarse[1].T, preferred_element_type=jnp.float32)
    lat_c = lat_c.reshape(height // 2, width // 2, -1).astype(jnp.bfloat16)
    results = []
    for level_index, lateral in enumerate((lat_a, lat_b, lat_c)):
        normed = channel_norm(lateral, norm_gain[2 * level_index], norm_shift[2 * level_index])
        convolved = conv_three(normed, output_conv[level_index])
        results.append(channel_norm(convolved, norm_gain[2 * level_index + 1], norm_shift[2 * level_index + 1]))
    level_sixty = results[2][::2, ::2]
    return (channel_major(results[0]), channel_major(results[1]), channel_major(results[2]), channel_major(level_sixty))
```

```python
import jax
import jax.numpy as jnp
from jax import lax
from jax.experimental import pallas as pl
from jax.experimental.pallas import tpu as pltpu
from jax.sharding import Mesh
from jax.sharding import PartitionSpec as P

MP = ("mp_0", "mp_1")
EPSILON = 1e-06
BF = jnp.bfloat16
F32 = jnp.float32
LANES = 128


def dot(a, b):
    return jnp.dot(a, b, preferred_element_type=F32)


def iota(shape, dim):
    return lax.broadcasted_iota(jnp.int32, shape, dim)


def one_hot(shape, source_of_column):
    rows = iota(shape, 0)
    columns = iota(shape, 1)
    return jnp.where(rows == source_of_column(columns), 1.0, 0.0).astype(BF)


def channel_norm(values, gain, shift):
    count = values.shape[0]
    center = jnp.sum(values, axis=0, keepdims=True) / count
    spread = jnp.sum(values * values, axis=0, keepdims=True) / count - center * center
    return (values - center) * lax.rsqrt(spread + EPSILON) * gain + shift


def spread_features(where, x, conv, lat, xb, wb):
    band = where[0]
    members = xb.shape[0]
    flat = x[...].astype(F32).T.astype(BF)
    for m in range(members):
        xb[m] = flat
    taps, rows, depth = conv.shape
    first = band == 0
    half = depth // 2
    own = conv[...].reshape(taps * rows, depth)
    own = jnp.where(first, own[:, :half], own[:, half:])
    lateral = lat[...]
    width = lateral.shape[1] // 2
    lateral = jnp.where(first, lateral[:, :width], lateral[:, width:])
    for m in range(members):
        wb[m, : taps * rows] = own
        for k in range(width // LANES):
            wb[m, taps * rows + k * rows : taps * rows + (k + 1) * rows] = lateral[
                :, k * LANES : (k + 1) * LANES
            ]


def raise_map(where, gathered, deconv, bias, coarse_w, rows_out, lat_out, edge_out):
    band = where[0]
    members, local, pixels = gathered.shape
    x = gathered[...].reshape(members * local, pixels)
    taps, half_local, depth = deconv.shape
    columns = pixels // (members // 2)
    raised = dot(deconv[...].reshape(taps * half_local, depth), x)
    diagonal = iota((half_local, half_local), 0) == iota((half_local, half_local), 1)
    bias_column = jnp.sum(jnp.where(diagonal, bias[...], 0.0), axis=1, keepdims=True)
    low = iota((half_local, LANES), 1) < columns
    for a in range(2):
        for p in range(pixels // LANES):
            tiles = [
                raised[
                    (2 * a + b) * half_local : (2 * a + b + 1) * half_local,
                    p * LANES : (p + 1) * LANES,
                ]
                + bias_column
                for b in range(2)
            ]
            swapped = [pltpu.roll(tile, columns, 1) for tile in tiles]
            rows_out[4 * p + a] = jnp.where(low, tiles[0], swapped[1]).astype(BF)
            rows_out[4 * p + 2 + a] = jnp.where(low, swapped[0], tiles[1]).astype(BF)
    middle = dot(coarse_w[0], x).astype(BF)
    floats = x.astype(F32)
    wide = jnp.maximum(floats, pltpu.roll(floats, pixels - 1, 1))
    pooled = jnp.maximum(wide, pltpu.roll(wide, pixels - columns, 1)).astype(BF)
    coarse = dot(coarse_w[1], pooled).astype(BF)
    small = columns // 2
    pick = one_hot(
        (pixels, LANES), lambda l: (l // small) * (2 * columns) + (l % small) * 2
    )
    coarse = dot(coarse, pick).astype(BF)
    lat_out[:, :pixels] = middle
    lat_out[:, pixels:] = coarse
    top = band == 0
    last = members - 1
    edge_out[:half_local] = jnp.where(top, rows_out[last], rows_out[0])
    tile = jnp.where(
        top,
        pltpu.roll(middle[:, pixels - LANES :].astype(F32), columns, 1),
        middle[:, :LANES].astype(F32),
    )
    floats = coarse.astype(F32)
    tail = jnp.where(top, pltpu.roll(floats, LANES - small, 1), pltpu.roll(floats, columns, 1))
    low = iota(tile.shape, 1) < columns
    edge_out[half_local:] = jnp.where(low, tile, tail).astype(BF)


def lay_out_rows(where, rows, lat, edge, out):
    band = where[0]
    members, half_local, _ = rows.shape
    neck_local = lat.shape[0]
    other = edge[:half_local]
    top = band == 0
    for m in range(members):
        above = rows[m - 1] if m > 0 else other
        below = rows[m + 1] if m < members - 1 else other
        out[m, :half_local] = above
        out[m, half_local : 2 * half_local] = rows[m]
        out[m, 2 * half_local : 3 * half_local] = below
        base = 3 * half_local
        for k in range(lat.shape[1] // LANES):
            out[m, base : base + neck_local] = lat[:, k * LANES : (k + 1) * LANES]
            base += neck_local
        out[m, base : base + neck_local] = edge[half_local:]


def small_conv(normed, halo, weight, width, band, halo_at):
    taps, out_local, depth = weight.shape
    stacked = weight.reshape(taps * out_local, depth)
    main = dot(stacked, normed)
    rim = dot(stacked, halo)
    cells = normed.shape[1]

    def across(values, r):
        size = values.shape[1]
        column = iota((out_local, size), 1) % width
        pieces = [
            values[(3 * r + q) * out_local : (3 * r + q + 1) * out_local] for q in range(3)
        ]
        left = jnp.where(column == 0, 0.0, pltpu.roll(pieces[0], 1, 1))
        right = jnp.where(column == width - 1, 0.0, pltpu.roll(pieces[2], size - 1, 1))
        return left + pieces[1] + right

    lane = iota((out_local, cells), 1)
    first = band == 0
    above = pltpu.roll(across(main, 0), width, 1)
    rim_above = pltpu.roll(across(rim, 0), (LANES - halo_at) % LANES, 1) if halo_at else across(rim, 0)
    rim_below = across(rim, 2)
    shift = (LANES - width - halo_at) % LANES
    if shift:
        rim_below = pltpu.roll(rim_below, shift, 1)
    if cells > LANES:
        blank = jnp.zeros((out_local, cells - LANES), F32)
        rim_above = jnp.concatenate([rim_above, blank], axis=1)
        rim_below = jnp.concatenate([blank, rim_below], axis=1)
    rim_above = jnp.where(first, 0.0, rim_above)
    rim_below = jnp.where(first, rim_below, 0.0)
    above = jnp.where(lane < width, rim_above, above)
    below = pltpu.roll(across(main, 2), cells - width, 1)
    below = jnp.where(lane >= cells - width, rim_below, below)
    return above + across(main, 1) + below


def levels(where, got, weights, weights_other, conv, gains, out, own_sixteen, own_thirty):
    band = where[0]
    row = where[1]
    members = got.shape[0]
    first_band = band == 0
    neck_local = conv.shape[2]
    neck = members * neck_local
    taps = conv.shape[1]
    half_local = (got.shape[1] - 6 * neck_local) // 3
    columns = LANES // 2

    def gain(index):
        return gains[:, index : index + 1], gains[:, 6 + index : 7 + index]

    mine = weights[...]
    other = weights_other[...]
    low = jnp.where(first_band, mine, other)
    high = jnp.where(first_band, other, mine)

    def weight_rows(source, index):
        return source[:, index * neck_local : (index + 1) * neck_local].reshape(neck, LANES)

    lateral = jnp.concatenate(
        [weight_rows(low, taps), weight_rows(low, taps + 1), weight_rows(high, taps), weight_rows(high, taps + 1)],
        axis=1,
    )
    raised = jnp.concatenate(
        [
            got[:, r * half_local : (r + 1) * half_local].reshape(members * half_local, LANES)
            for r in range(3)
        ],
        axis=1,
    )
    lat = dot(lateral, raised).astype(BF).astype(F32)
    normed = channel_norm(lat, *gain(0))
    lane = iota((neck, LANES), 1)
    odd = lane >= columns
    total = jnp.zeros((neck, LANES), F32)
    for r in range(3):
        center = normed[:, r * LANES : (r + 1) * LANES]
        if r == 0:
            center = jnp.where(first_band & (row == 0), 0.0, center)
        if r == 2:
            center = jnp.where(jnp.logical_not(first_band) & (row == members - 1), 0.0, center)
        swapped = pltpu.roll(center, columns, 1)
        left = jnp.where(odd, swapped, pltpu.roll(swapped, 1, 1))
        left = jnp.where(lane == 0, 0.0, left)
        right = jnp.where(odd, pltpu.roll(swapped, LANES - 1, 1), swapped)
        right = jnp.where(lane == LANES - 1, 0.0, right)
        for q, window in enumerate((left, center, right)):
            tap = jnp.concatenate([weight_rows(low, 3 * r + q), weight_rows(high, 3 * r + q)], axis=1)
            total = total + dot(tap, window.astype(BF))
    convolved = total.astype(BF).astype(F32)
    level = channel_norm(convolved, *gain(1)).astype(BF)
    mix = one_hot((LANES, LANES), lambda l: (l % 2) * columns + l // 2)
    out[:, :neck_local] = dot(level, mix).reshape(members, neck_local, LANES)

    def tile(k):
        base = 3 * half_local + k * neck_local
        return got[:, base : base + neck_local].reshape(neck, LANES).astype(F32)

    middle = jnp.concatenate([tile(k) for k in range(4)], axis=1)
    rim = tile(5)
    gain_two, shift_two = gain(2)
    sixteen = small_conv(
        channel_norm(middle, gain_two, shift_two).astype(BF),
        channel_norm(rim, gain_two, shift_two).astype(BF),
        conv[1], columns, band, 0,
    ).astype(BF)
    gain_four, shift_four = gain(4)
    thirty = small_conv(
        channel_norm(tile(4), gain_four, shift_four).astype(BF),
        channel_norm(rim, gain_four, shift_four).astype(BF),
        conv[2], columns // 2, band, columns,
    ).astype(BF)
    own_sixteen[...] = sixteen
    own_thirty[...] = thirty
    floats = jnp.concatenate([sixteen, thirty], axis=1).astype(F32)
    sums = jnp.sum(floats, axis=0, keepdims=True)
    squares = jnp.sum(floats * floats, axis=0, keepdims=True)
    pieces = floats.shape[1] // LANES
    stats = jnp.concatenate(
        [part[:, k * LANES : (k + 1) * LANES] for part in (sums, squares) for k in range(pieces)]
        + [jnp.zeros((neck_local - 2 * pieces, LANES), F32)],
        axis=0,
    )
    for m in range(members):
        out[m, neck_local:] = stats


def finish(where, got, own_sixteen, own_thirty, gains, eight, sixteen, thirty, sixty):
    row = where[1]
    members = got.shape[0]
    neck_local = own_sixteen.shape[0]
    neck = members * neck_local
    for m in range(members):
        eight[:, m * LANES : (m + 1) * LANES] = got[m, :neck_local].astype(BF)
    stats = jnp.sum(got[:, neck_local:], axis=0) / neck
    start = pl.multiple_of(row * neck_local, neck_local)
    own = gains[pl.ds(start, neck_local), :]
    pieces = own_sixteen.shape[1] // LANES + 1

    def apply(values, k, index):
        center = stats[k : k + 1]
        spread = stats[pieces + k : pieces + k + 1] - center * center
        return (
            (values.astype(F32) - center) * lax.rsqrt(spread + EPSILON) * own[:, index : index + 1]
            + own[:, 6 + index : 7 + index]
        ).astype(BF)

    for k in range(pieces - 1):
        at = slice(k * LANES, (k + 1) * LANES)
        sixteen[:, at] = apply(own_sixteen[:, at], k, 3)
    last = apply(own_thirty[...], pieces - 1, 5)
    thirty[...] = last
    small = LANES // 4
    cells = sixty.shape[1]
    pick = one_hot(
        (LANES, cells), lambda l: (l // (small // 2)) * (2 * small) + (l % (small // 2)) * 2
    )
    sixty[...] = dot(last, pick).astype(BF)


def call(kernel, outs, where, *operands):
    specs = [pl.BlockSpec(memory_space=pltpu.SMEM)] + [
        pl.BlockSpec(memory_space=pltpu.VMEM) for _ in operands
    ]
    return pl.pallas_call(
        kernel,
        in_specs=specs,
        out_specs=jax.tree.map(lambda _: pl.BlockSpec(memory_space=pltpu.VMEM), outs),
        out_shape=outs,
        name=kernel.__name__,
    )(where, *operands)


def per_device(
    features,
    deconv_weight,
    deconv_bias,
    lateral_eight,
    lateral_coarse,
    output_conv,
    norm_gain,
    norm_shift,
):
    row_count, col_count, local = features.shape
    members = lax.axis_size(MP)
    pixels = row_count * col_count
    half_local = deconv_weight.shape[1]
    neck_local = lateral_eight.shape[0]
    neck = members * neck_local
    shape = jax.ShapeDtypeStruct
    where = jnp.stack([lax.axis_index("space"), lax.axis_index(MP)]).astype(jnp.int32)
    gains = jnp.concatenate([norm_gain, norm_shift], axis=0).T
    conv = output_conv.transpose(0, 2, 1, 3)
    weight_rows = 11 * neck_local
    swap = [(0, 1), (1, 0)]

    xb, wb = call(
        spread_features,
        (shape((members, local, pixels), BF), shape((members, weight_rows, LANES), BF)),
        where, features.reshape(pixels, local), conv[0], lateral_eight,
    )
    gathered = lax.all_to_all(xb, MP, 0, 0, tiled=True)
    weights = lax.all_to_all(wb, MP, 0, 0, tiled=True)
    weights_other = lax.ppermute(weights, "space", swap)
    rows, lat, edge = call(
        raise_map,
        (
            shape((members, half_local, LANES), BF),
            shape((neck_local, pixels + LANES), BF),
            shape((half_local + neck_local, LANES), BF),
        ),
        where, gathered, deconv_weight, deconv_bias.reshape(1, half_local), lateral_coarse,
    )
    edge = lax.ppermute(edge, "space", swap)
    blocks = call(
        lay_out_rows,
        shape((members, 3 * half_local + 6 * neck_local, LANES), BF),
        where, rows, lat, edge,
    )
    got = lax.all_to_all(blocks, MP, 0, 0, tiled=True)
    blocks, own_sixteen, own_thirty = call(
        levels,
        (
            shape((members, 2 * neck_local, LANES), F32),
            shape((neck_local, pixels), BF),
            shape((neck_local, pixels // 4), BF),
        ),
        where, got, weights, weights_other, conv, gains,
    )
    got = lax.all_to_all(blocks, MP, 0, 0, tiled=True)
    return call(
        finish,
        (
            shape((neck_local, 4 * pixels), BF),
            shape((neck_local, pixels), BF),
            shape((neck_local, pixels // 4), BF),
            shape((neck_local, pixels // 16), BF),
        ),
        where, got, own_sixteen, own_thirty, gains,
    )


def solution(mesh):
    finer = Mesh(
        mesh.devices.reshape(mesh.shape["dp"], mesh.shape["space"], 4, 4),
        ("dp", "space", "mp_0", "mp_1"),
    )
    in_specs = (
        P(("dp", "space"), None, MP),
        P(None, MP, None),
        P(MP),
        P(MP, None),
        P(None, MP, None),
        P(None, MP, None, None),
        P(),
        P(),
    )
    return jax.shard_map(
        per_device,
        mesh=finer,
        in_specs=in_specs,
        out_specs=(P(MP, ("dp", "space")),) * 4,
        check_vma=False,
    )
```

```python
import jax
import jax.numpy as jnp
from jax import lax
from jax.experimental import pallas as pl
from jax.experimental.pallas import tpu as pltpu
from jax.sharding import Mesh
from jax.sharding import PartitionSpec as P

MP = ("mp_0", "mp_1")
EPSILON = 1e-06
BF = jnp.bfloat16
F32 = jnp.float32
LANES = 128
GRANT = 12 * 1024 * 1024
NECK_ROWS = 16


def dot(a, b):
    return jnp.dot(a, b, preferred_element_type=F32)


def iota(shape, dim):
    return lax.broadcasted_iota(jnp.int32, shape, dim)


def one_hot(shape, source_of_column):
    rows = iota(shape, 0)
    columns = iota(shape, 1)
    return jnp.where(rows == source_of_column(columns), 1.0, 0.0).astype(BF)


def channel_norm(values, gain, shift):
    count = values.shape[0]
    center = jnp.sum(values, axis=0, keepdims=True) / count
    spread = jnp.sum(values * values, axis=0, keepdims=True) / count - center * center
    return (values - center) * lax.rsqrt(spread + EPSILON) * gain + shift


def weight_piece(block, base, index):
    members = block.shape[0]
    rows = NECK_ROWS
    start = base + rows * (index // 4)
    lane = LANES * (index % 4)
    return block[:, start : start + rows, lane : lane + LANES].reshape(members * rows, LANES)


def spread_features(band_at, row_at, x, conv, lat, out):
    members = out.shape[0]
    local = x.shape[1]
    first = band_at[0] == 0
    flat = x[...].astype(F32).T.astype(BF)
    taps = conv.shape[1]
    half = conv.shape[3] // 2
    pieces = [jnp.where(first, conv[0, t, :, :half], conv[0, t, :, half:]) for t in range(taps)]
    half = lat.shape[1] // 2
    lateral = jnp.where(first, lat[:, :half], lat[:, half:])
    pieces += [lateral[:, :LANES], lateral[:, LANES:], jnp.zeros_like(pieces[0])]
    weights = jnp.concatenate(
        [jnp.concatenate(pieces[k : k + 4], axis=1) for k in range(0, len(pieces), 4)], axis=0
    )
    for m in range(members):
        out[m, :local] = flat
        out[m, local:] = weights


def raise_map(band_at, row_at, gathered, deconv, bias, coarse_w, out, rows):
    members = gathered.shape[0]
    pixels = gathered.shape[2]
    taps, half_local, depth = deconv.shape
    local = depth // members
    x = gathered[:, :local].reshape(depth, pixels)
    columns = 2 * pixels // members
    small = columns // 2
    raised = dot(deconv[...].reshape(taps * half_local, depth), x)
    diagonal = iota((half_local, half_local), 0) == iota((half_local, half_local), 1)
    bias_column = jnp.sum(jnp.where(diagonal, bias[...], 0.0), axis=1, keepdims=True)
    low = iota((half_local, LANES), 1) < columns
    for a in range(2):
        for p in range(pixels // LANES):
            tiles = [
                raised[
                    (2 * a + b) * half_local : (2 * a + b + 1) * half_local,
                    p * LANES : (p + 1) * LANES,
                ]
                + bias_column
                for b in range(2)
            ]
            swapped = [pltpu.roll(tile, columns, 1) for tile in tiles]
            rows[4 * p + a] = jnp.where(low, tiles[0], swapped[1]).astype(BF)
            rows[4 * p + 2 + a] = jnp.where(low, swapped[0], tiles[1]).astype(BF)
    middle = dot(coarse_w[0], x).astype(BF)
    low = iota((depth, LANES), 1) < columns
    pairs = []
    for p in range(pixels // LANES):
        tile = x[:, p * LANES : (p + 1) * LANES].astype(F32)
        pairs.append(jnp.maximum(tile, pltpu.roll(tile, columns, 1)))
    packed = []
    for p in range(0, len(pairs), 2):
        both = jnp.where(low, pairs[p], pairs[p + 1])
        packed.append(jnp.maximum(both, pltpu.roll(both, LANES - 1, 1)).astype(BF))
    coarse = dot(coarse_w[1], jnp.concatenate(packed, axis=1)).astype(BF)
    coarse = dot(coarse, one_hot((pixels // 2, LANES), lambda l: 2 * l)).astype(BF)
    tail = [middle[:, p * LANES : (p + 1) * LANES] for p in range(pixels // LANES)] + [coarse]
    tail = jnp.concatenate(tail, axis=0)
    first = band_at[0] == 0
    for m in range(members):
        row = jnp.where(first, m, members - 1 - m)
        for k in range(3):
            out[m, k * half_local : (k + 1) * half_local] = rows[
                jnp.clip(row + k - 1, 0, members - 1)
            ]
        out[m, 3 * half_local :] = tail


def columns_of(gain, shift):
    blank = jnp.zeros((2, gain.shape[1]), F32)
    return jnp.concatenate([gain[...], blank, shift[...], blank], axis=0).T


def scaled(table, index):
    return table[:, index : index + 1], table[:, 8 + index : 9 + index]


def lateral_weight(low, high, base):
    return jnp.concatenate(
        [weight_piece(block, base, 9 + k) for block in (low, high) for k in range(2)], axis=1
    )


def windows(center):
    lane = iota(center.shape, 1)
    columns = LANES // 2
    odd = lane >= columns
    swapped = pltpu.roll(center, columns, 1)
    left = jnp.where(odd, swapped, pltpu.roll(swapped, 1, 1))
    left = jnp.where(lane == 0, 0.0, left)
    right = jnp.where(odd, pltpu.roll(swapped, LANES - 1, 1), swapped)
    right = jnp.where(lane == LANES - 1, 0.0, right)
    return [window.astype(BF) for window in (left, center, right)]


def level_eight(band_at, row_at, got, gathered, other, gain, shift, total_out):
    members = got.shape[0]
    first = band_at[0] == 0
    row = jnp.where(first, row_at[0], members - 1 - row_at[0])
    local = gathered.shape[1] - 3 * NECK_ROWS
    half_local = (got.shape[1] - 5 * NECK_ROWS) // 3
    table = columns_of(gain, shift)
    mine = gathered[:, local:]
    theirs = other[:, local:]
    low = jnp.where(first, mine, theirs)
    high = jnp.where(first, theirs, mine)
    raised = jnp.concatenate(
        [
            got[:, r * half_local : (r + 1) * half_local].reshape(members * half_local, LANES)
            for r in range(3)
        ],
        axis=1,
    )
    lat = dot(lateral_weight(low, high, 0), raised).astype(BF).astype(F32)
    normed = channel_norm(lat, *scaled(table, 0))
    total = None
    for r in range(3):
        center = normed[:, r * LANES : (r + 1) * LANES]
        if r == 0:
            center = jnp.where(row == 0, 0.0, center)
        if r == 2:
            center = jnp.where(row == members - 1, 0.0, center)
        for q, window in enumerate(windows(center)):
            tap = jnp.concatenate(
                [weight_piece(block, 0, 3 * r + q) for block in (low, high)], axis=1
            )
            part = dot(tap, window)
            total = part if total is None else total + part
    total_out[...] = total


def small_conv(normed, halo, weight, width, first):
    taps, out_local, depth = weight.shape
    stacked = weight.reshape(taps * out_local, depth)
    main = dot(stacked, normed)
    rim = dot(stacked, halo)
    cells = normed.shape[1]

    def across(values, r):
        size = values.shape[1]
        column = iota((out_local, size), 1) % width
        pieces = [
            values[(3 * r + q) * out_local : (3 * r + q + 1) * out_local] for q in range(3)
        ]
        left = jnp.where(column == 0, 0.0, pltpu.roll(pieces[0], 1, 1))
        right = jnp.where(column == width - 1, 0.0, pltpu.roll(pieces[2], size - 1, 1))
        return left + pieces[1] + right

    lane = iota((out_local, cells), 1)
    rim_above = jnp.where(first, 0.0, across(rim, 0))
    rim_below = jnp.where(first, pltpu.roll(across(rim, 2), LANES - width, 1), 0.0)
    if cells > LANES:
        blank = jnp.zeros((out_local, cells - LANES), F32)
        rim_above = jnp.concatenate([rim_above, blank], axis=1)
        rim_below = jnp.concatenate([blank, rim_below], axis=1)
    above = jnp.where(lane < width, rim_above, pltpu.roll(across(main, 0), width, 1))
    below = jnp.where(
        lane >= cells - width, rim_below, pltpu.roll(across(main, 2), cells - width, 1)
    )
    return above + across(main, 1) + below


def levels(
    band_at, row_at, got, got_other, total, gathered, other, conv, gain, shift,
    out, own_sixteen, own_thirty, own_table, table_at,
):
    members = got.shape[0]
    first = band_at[0] == 0
    neck = members * NECK_ROWS
    local = gathered.shape[1] - 3 * NECK_ROWS
    half_local = (got.shape[1] - 5 * NECK_ROWS) // 3
    columns = LANES // 2
    table = columns_of(gain, shift)
    table_at[...] = table
    start = pl.multiple_of(row_at[0] * NECK_ROWS, NECK_ROWS)
    own_table[...] = table_at[pl.ds(start, NECK_ROWS), :]

    mine = gathered[:, local:]
    theirs = other[:, local:]
    low = jnp.where(first, mine, theirs)
    high = jnp.where(first, theirs, mine)
    raised = got_other[:, half_local : 2 * half_local].reshape(members * half_local, LANES)
    lat = dot(lateral_weight(low, high, 0), raised).astype(BF).astype(F32)
    center = channel_norm(lat, *scaled(table, 0))
    center = jnp.where(row_at[0] == members - 1, center, 0.0)
    convolved = total[...]
    for q, window in enumerate(windows(center)):
        tap = jnp.concatenate(
            [
                jnp.where(first, weight_piece(block, 0, 6 + q), weight_piece(block, 0, q))
                for block in (low, high)
            ],
            axis=1,
        )
        convolved = convolved + dot(tap, window)
    convolved = convolved.astype(BF).astype(F32)
    level = channel_norm(convolved, *scaled(table, 1)).astype(BF)
    mix = one_hot((LANES, LANES), lambda l: (l % 2) * columns + l // 2)
    out[:, :NECK_ROWS] = dot(level, mix).astype(BF).reshape(members, NECK_ROWS, LANES)

    def tile(source, k):
        base = 3 * half_local + k * NECK_ROWS
        return source[:, base : base + NECK_ROWS].reshape(neck, LANES).astype(F32)

    middle = jnp.concatenate([tile(got, k) for k in range(4)], axis=1)
    rim = jnp.where(first, tile(got_other, 0), pltpu.roll(tile(got_other, 3), columns, 1))
    sixteen = small_conv(
        channel_norm(middle, *scaled(table, 2)).astype(BF),
        channel_norm(rim, *scaled(table, 2)).astype(BF),
        conv[1], columns, first,
    ).astype(BF)
    rim = tile(got_other, 4)
    rim = jnp.where(first, rim, pltpu.roll(rim, columns // 2, 1))
    thirty = small_conv(
        channel_norm(tile(got, 4), *scaled(table, 4)).astype(BF),
        channel_norm(rim, *scaled(table, 4)).astype(BF),
        conv[2], columns // 2, first,
    ).astype(BF)
    own_sixteen[...] = sixteen
    own_thirty[...] = thirty
    floats = jnp.concatenate([sixteen, thirty], axis=1).astype(F32)
    sums = jnp.sum(floats, axis=0, keepdims=True)
    squares = jnp.sum(floats * floats, axis=0, keepdims=True)
    pieces = floats.shape[1] // LANES
    stats = jnp.concatenate(
        [part[:, k * LANES : (k + 1) * LANES] for part in (sums, squares) for k in range(pieces)]
        + [jnp.zeros((NECK_ROWS - 2 * pieces, LANES), F32)],
        axis=0,
    )
    parts = []
    for _ in range(3):
        parts.append(stats.astype(BF))
        stats = stats - parts[-1].astype(F32)
    parts = jnp.concatenate(parts, axis=0)
    for m in range(members):
        out[m, NECK_ROWS:] = parts


def finish(band_at, row_at, got, own_sixteen, own_thirty, table, eight, sixteen, thirty, sixty):
    members = got.shape[0]
    first = band_at[0] == 0
    neck = members * NECK_ROWS
    for r in range(members):
        source = jnp.where(first, r, members - 1 - r)
        eight[:, r * LANES : (r + 1) * LANES] = got[source, :NECK_ROWS]
    stats = jnp.sum(got[:, NECK_ROWS:].astype(F32), axis=0)
    stats = stats[:NECK_ROWS] + stats[NECK_ROWS : 2 * NECK_ROWS] + stats[2 * NECK_ROWS :]
    stats = stats / neck
    pieces = own_sixteen.shape[1] // LANES + 1

    def apply(values, k, index):
        gain, shift = scaled(table, index)
        center = stats[k : k + 1]
        spread = stats[pieces + k : pieces + k + 1] - center * center
        return ((values.astype(F32) - center) * lax.rsqrt(spread + EPSILON) * gain + shift).astype(BF)

    for k in range(pieces - 1):
        at = slice(k * LANES, (k + 1) * LANES)
        sixteen[:, at] = apply(own_sixteen[:, at], k, 3)
    last = apply(own_thirty[...], pieces - 1, 5)
    thirty[...] = last
    small = LANES // 4
    pick = one_hot(
        (LANES, sixty.shape[1]),
        lambda l: (l // (small // 2)) * (2 * small) + (l % (small // 2)) * 2,
    )
    sixty[...] = dot(last, pick).astype(BF)


def call(kernel, outs, where, *operands, scratch=()):
    specs = [pl.BlockSpec(memory_space=pltpu.SMEM) for _ in where] + [
        pl.BlockSpec(memory_space=pltpu.VMEM) for _ in operands
    ]
    return pl.pallas_call(
        kernel,
        in_specs=specs,
        out_specs=jax.tree.map(lambda _: pl.BlockSpec(memory_space=pltpu.VMEM), outs),
        out_shape=outs,
        scratch_shapes=scratch,
        name=kernel.__name__,
        compiler_params=pltpu.CompilerParams(vmem_limit_bytes=GRANT),
    )(*where, *operands)


def per_device(
    features,
    deconv_weight,
    deconv_bias,
    lateral_eight,
    lateral_coarse,
    output_conv,
    norm_gain,
    norm_shift,
):
    row_count, col_count, local = features.shape
    members = lax.axis_size(MP)
    pixels = row_count * col_count
    half_local = deconv_weight.shape[1]
    neck = norm_gain.shape[1]
    assert members == 2 * row_count and 2 * col_count == LANES
    assert lateral_eight.shape[0] == NECK_ROWS and members * NECK_ROWS == neck
    shape = jax.ShapeDtypeStruct
    where = [lax.axis_index(axis).astype(jnp.int32).reshape(1) for axis in ("space", MP)]
    conv = output_conv.transpose(0, 2, 1, 3)
    swap = [(0, 1), (1, 0)]

    blocks = call(
        spread_features,
        shape((members, local + 3 * NECK_ROWS, pixels), BF),
        where, features.reshape(pixels, local), conv, lateral_eight,
    )
    gathered = lax.all_to_all(blocks, MP, 0, 0, tiled=True)
    other = lax.ppermute(gathered, "space", swap)
    blocks = call(
        raise_map,
        shape((members, 3 * half_local + 5 * NECK_ROWS, LANES), BF),
        where, gathered, deconv_weight, deconv_bias.reshape(1, half_local), lateral_coarse,
        scratch=[pltpu.VMEM((members, half_local, LANES), BF)],
    )
    got = lax.all_to_all(blocks, MP, 0, 0, tiled=True)
    got_other = lax.ppermute(got, "space", swap)
    total = call(
        level_eight, shape((neck, LANES), F32),
        where, got, gathered, other, norm_gain, norm_shift,
    )
    blocks, own_sixteen, own_thirty, table = call(
        levels,
        (
            shape((members, 4 * NECK_ROWS, LANES), BF),
            shape((NECK_ROWS, pixels), BF),
            shape((NECK_ROWS, pixels // 4), BF),
            shape((NECK_ROWS, 16), F32),
        ),
        where, got, got_other, total, gathered, other, conv, norm_gain, norm_shift,
        scratch=[pltpu.VMEM((neck, 16), F32)],
    )
    got = lax.all_to_all(blocks, MP, 0, 0, tiled=True)
    return call(
        finish,
        (
            shape((NECK_ROWS, 4 * pixels), BF),
            shape((NECK_ROWS, pixels), BF),
            shape((NECK_ROWS, pixels // 4), BF),
            shape((NECK_ROWS, pixels // 16), BF),
        ),
        where, got, own_sixteen, own_thirty, table,
    )


def solution(mesh):
    finer = Mesh(
        mesh.devices.reshape(mesh.shape["dp"], mesh.shape["space"], 4, 4),
        ("dp", "space", "mp_0", "mp_1"),
    )
    in_specs = (
        P(("dp", "space"), None, MP),
        P(None, MP, None),
        P(MP),
        P(MP, None),
        P(None, MP, None),
        P(None, MP, None, None),
        P(),
        P(),
    )
    return jax.shard_map(
        per_device,
        mesh=finer,
        in_specs=in_specs,
        out_specs=(P(MP, ("dp", "space")),) * 4,
        check_vma=False,
    )
```

```python
import jax
import jax.numpy as jnp
from jax import lax
from jax.experimental import pallas as pl
from jax.experimental.pallas import tpu as pltpu
from jax.sharding import Mesh
from jax.sharding import PartitionSpec as P


MP = ("mp_0", "mp_1")
EPSILON = 1e-06
BF = jnp.bfloat16
F32 = jnp.float32
LANES = 128
GRANT = 12 * 1024 * 1024
NECK_ROWS = 16
SHARES = 2
PER_SHARE = 6


def dot(a, b):
    return jnp.dot(a, b, preferred_element_type=F32)


def iota(shape, dim):
    return lax.broadcasted_iota(jnp.int32, shape, dim)


def one_hot(shape, source_of_column):
    rows = iota(shape, 0)
    columns = iota(shape, 1)
    return jnp.where(rows == source_of_column(columns), 1.0, 0.0).astype(BF)


def channel_norm(values, gain, shift):
    count = values.shape[0]
    center = jnp.sum(values, axis=0, keepdims=True) / count
    spread = jnp.sum(values * values, axis=0, keepdims=True) / count - center * center
    return (values - center) * lax.rsqrt(spread + EPSILON) * gain + shift


def weight_piece(halves, index):
    share, at = index // PER_SHARE, index % PER_SHARE
    return jnp.concatenate(
        [
            half[share, :, at * NECK_ROWS : (at + 1) * NECK_ROWS].reshape(-1, LANES)
            for half in halves
        ],
        axis=1,
    )


def spread_features(
    band_at, parity_at, x_from, conv_from, lat_from, out, x, conv, lat, arrived
):
    copies = [
        pltpu.make_async_copy(x_from, x, arrived.at[0]),
        pltpu.make_async_copy(conv_from.at[0], conv, arrived.at[1]),
        pltpu.make_async_copy(lat_from, lat, arrived.at[2]),
    ]
    for copy in copies:
        copy.start()
    for copy in copies:
        copy.wait()
    members = out.shape[0]
    first = band_at[0] == 0
    even = parity_at[0] == 0
    flat = x[...].astype(F32).T.astype(BF)
    flat = jnp.concatenate(
        [flat[:, k : k + LANES] for k in range(0, flat.shape[1], LANES)], axis=0
    )
    half = lat.shape[1] // 2
    lateral = jnp.where(first, lat[:, :half], lat[:, half:])
    pieces = [jnp.where(first, conv[t, :, :LANES], conv[t, :, LANES:]) for t in range(9)]
    pieces += [lateral[:, :LANES], lateral[:, LANES:], lateral[:, LANES:]]
    weights = [jnp.where(even, pieces[k], pieces[PER_SHARE + k]) for k in range(PER_SHARE)]
    weights = jnp.concatenate(weights, axis=0)
    start = flat.shape[0]
    for m in range(members):
        out[m, :start] = flat
        out[m, start:] = weights


def raise_map(band_at, gathered, deconv, bias, coarse_w, out, share, share_low, share_high, rows):
    members = gathered.shape[0]
    taps, half_local, depth = deconv.shape
    local = depth // members
    weight_rows = share.shape[1]
    split = gathered.shape[1] - weight_rows
    pixels = split // local * LANES
    half = members // 2
    share[...] = gathered[:, split:]
    share_low[...] = gathered[:half, split:]
    share_high[...] = gathered[half:, split:]
    x = jnp.concatenate(
        [gathered[:, k : k + local].reshape(depth, LANES) for k in range(0, split, local)], axis=1
    )
    columns = 2 * pixels // members
    raised = dot(deconv[...].reshape(taps * half_local, depth), x)
    diagonal = iota((half_local, half_local), 0) == iota((half_local, half_local), 1)
    bias_column = jnp.sum(jnp.where(diagonal, bias[...], 0.0), axis=1, keepdims=True)
    low = iota((half_local, LANES), 1) < columns
    for a in range(2):
        for p in range(pixels // LANES):
            tiles = [
                raised[
                    (2 * a + b) * half_local : (2 * a + b + 1) * half_local,
                    p * LANES : (p + 1) * LANES,
                ]
                + bias_column
                for b in range(2)
            ]
            swapped = [pltpu.roll(tile, columns, 1) for tile in tiles]
            rows[4 * p + a] = jnp.where(low, tiles[0], swapped[1]).astype(BF)
            rows[4 * p + 2 + a] = jnp.where(low, swapped[0], tiles[1]).astype(BF)
    middle = dot(coarse_w[0], x).astype(BF)
    low = iota((depth, LANES), 1) < columns
    pairs = []
    for p in range(pixels // LANES):
        tile = x[:, p * LANES : (p + 1) * LANES].astype(F32)
        pairs.append(jnp.maximum(tile, pltpu.roll(tile, columns, 1)))
    packed = []
    for p in range(0, len(pairs), 2):
        both = jnp.where(low, pairs[p], pairs[p + 1])
        packed.append(jnp.maximum(both, pltpu.roll(both, LANES - 1, 1)).astype(BF))
    coarse = dot(coarse_w[1], jnp.concatenate(packed, axis=1)).astype(BF)
    coarse = dot(coarse, one_hot((pixels // 2, LANES), lambda l: 2 * l)).astype(BF)
    tail = [middle[:, p * LANES : (p + 1) * LANES] for p in range(pixels // LANES)] + [coarse]
    tail = jnp.concatenate(tail, axis=0)
    first = band_at[0] == 0
    for m in range(members):
        row = jnp.where(first, m, members - 1 - m)
        for k in range(3):
            out[m, k * half_local : (k + 1) * half_local] = rows[
                jnp.clip(row + k - 1, 0, members - 1)
            ]
        out[m, 3 * half_local :] = tail


def columns_of(gain, shift):
    blank = jnp.zeros((2, gain.shape[1]), F32)
    return jnp.concatenate([gain[...], blank, shift[...], blank], axis=0).T


def scaled(table, index):
    return table[:, index : index + 1], table[:, 8 + index : 9 + index]


def merge_shares(parity_at, own, low, high, out):
    parity = parity_at[0]
    middle = low.shape[0]
    out[parity] = own[...]
    out[1 - parity, :middle] = low[...]
    out[1 - parity, middle:] = high[...]


def lateral_weight(halves):
    pair = [weight_piece([half], 9 + k) for half in halves for k in range(2)]
    return jnp.concatenate(pair, axis=1)


def windows(center):
    lane = iota(center.shape, 1)
    columns = LANES // 2
    odd = lane >= columns
    swapped = pltpu.roll(center, columns, 1)
    left = jnp.where(odd, swapped, pltpu.roll(swapped, 1, 1))
    left = jnp.where(lane == 0, 0.0, left)
    right = jnp.where(odd, pltpu.roll(swapped, LANES - 1, 1), swapped)
    right = jnp.where(lane == LANES - 1, 0.0, right)
    return [window.astype(BF) for window in (left, center, right)]


def ordered_halves(first, mine, theirs):
    low = jnp.where(first, mine[...], theirs[...])
    high = jnp.where(first, theirs[...], mine[...])
    return low, high


def level_eight(band_at, row_at, got, mine, theirs, gain, shift, total_out):
    members = got.shape[0]
    first = band_at[0] == 0
    row = jnp.where(first, row_at[0], members - 1 - row_at[0])
    half_local = (got.shape[1] - 5 * NECK_ROWS) // 3
    table = columns_of(gain, shift)
    halves = ordered_halves(first, mine, theirs)
    raised = jnp.concatenate(
        [
            got[:, r * half_local : (r + 1) * half_local].reshape(members * half_local, LANES)
            for r in range(3)
        ],
        axis=1,
    )
    lat = dot(lateral_weight(halves), raised).astype(BF).astype(F32)
    normed = channel_norm(lat, *scaled(table, 0))
    total = None
    for r in range(3):
        center = normed[:, r * LANES : (r + 1) * LANES]
        if r == 0:
            center = jnp.where(row == 0, 0.0, center)
        if r == 2:
            center = jnp.where(row == members - 1, 0.0, center)
        for q, window in enumerate(windows(center)):
            part = dot(weight_piece(halves, 3 * r + q), window)
            total = part if total is None else total + part
    total_out[...] = total


def small_conv(normed, halo, weight, width, first):
    taps, out_local, depth = weight.shape
    stacked = weight.reshape(taps * out_local, depth)
    main = dot(stacked, normed)
    rim = dot(stacked, halo)
    cells = normed.shape[1]

    def across(values, r):
        size = values.shape[1]
        column = iota((out_local, size), 1) % width
        pieces = [
            values[(3 * r + q) * out_local : (3 * r + q + 1) * out_local] for q in range(3)
        ]
        left = jnp.where(column == 0, 0.0, pltpu.roll(pieces[0], 1, 1))
        right = jnp.where(column == width - 1, 0.0, pltpu.roll(pieces[2], size - 1, 1))
        return left + pieces[1] + right

    lane = iota((out_local, cells), 1)
    rim_above = jnp.where(first, 0.0, across(rim, 0))
    rim_below = jnp.where(first, pltpu.roll(across(rim, 2), LANES - width, 1), 0.0)
    if cells > LANES:
        blank = jnp.zeros((out_local, cells - LANES), F32)
        rim_above = jnp.concatenate([rim_above, blank], axis=1)
        rim_below = jnp.concatenate([blank, rim_below], axis=1)
    above = jnp.where(lane < width, rim_above, pltpu.roll(across(main, 0), width, 1))
    below = jnp.where(
        lane >= cells - width, rim_below, pltpu.roll(across(main, 2), cells - width, 1)
    )
    return above + across(main, 1) + below


def levels(
    band_at, row_at, got, got_other, total, mine, theirs, conv, gain, shift,
    out, own_sixteen, own_thirty, own_table, table_at,
):
    members = got.shape[0]
    first = band_at[0] == 0
    neck = members * NECK_ROWS
    half_local = (got.shape[1] - 5 * NECK_ROWS) // 3
    columns = LANES // 2
    table = columns_of(gain, shift)
    table_at[...] = table
    start = pl.multiple_of(row_at[0] * NECK_ROWS, NECK_ROWS)
    own_table[...] = table_at[pl.ds(start, NECK_ROWS), :]

    halves = ordered_halves(first, mine, theirs)
    raised = got_other[:, half_local : 2 * half_local].reshape(members * half_local, LANES)
    lat = dot(lateral_weight(halves), raised).astype(BF).astype(F32)
    center = channel_norm(lat, *scaled(table, 0))
    center = jnp.where(row_at[0] == members - 1, center, 0.0)
    convolved = total[...]
    for q, window in enumerate(windows(center)):
        tap = jnp.where(first, weight_piece(halves, 6 + q), weight_piece(halves, q))
        convolved = convolved + dot(tap, window)
    convolved = convolved.astype(BF).astype(F32)
    level = channel_norm(convolved, *scaled(table, 1)).astype(BF)
    mix = one_hot((LANES, LANES), lambda l: (l % 2) * columns + l // 2)
    out[:, :NECK_ROWS] = dot(level, mix).astype(BF).reshape(members, NECK_ROWS, LANES)

    def tile(source, k):
        base = 3 * half_local + k * NECK_ROWS
        return source[:, base : base + NECK_ROWS].reshape(neck, LANES).astype(F32)

    middle = jnp.concatenate([tile(got, k) for k in range(4)], axis=1)
    rim = jnp.where(first, tile(got_other, 0), pltpu.roll(tile(got_other, 3), columns, 1))
    sixteen = small_conv(
        channel_norm(middle, *scaled(table, 2)).astype(BF),
        channel_norm(rim, *scaled(table, 2)).astype(BF),
        conv[1], columns, first,
    ).astype(BF)
    rim = tile(got_other, 4)
    rim = jnp.where(first, rim, pltpu.roll(rim, columns // 2, 1))
    thirty = small_conv(
        channel_norm(tile(got, 4), *scaled(table, 4)).astype(BF),
        channel_norm(rim, *scaled(table, 4)).astype(BF),
        conv[2], columns // 2, first,
    ).astype(BF)
    own_sixteen[...] = sixteen
    own_thirty[...] = thirty
    floats = jnp.concatenate([sixteen, thirty], axis=1).astype(F32)
    sums = jnp.sum(floats, axis=0, keepdims=True)
    squares = jnp.sum(floats * floats, axis=0, keepdims=True)
    pieces = floats.shape[1] // LANES
    stats = jnp.concatenate(
        [part[:, k * LANES : (k + 1) * LANES] for part in (sums, squares) for k in range(pieces)]
        + [jnp.zeros((NECK_ROWS - 2 * pieces, LANES), F32)],
        axis=0,
    )
    parts = []
    for _ in range(3):
        parts.append(stats.astype(BF))
        stats = stats - parts[-1].astype(F32)
    parts = jnp.concatenate(parts, axis=0)
    for m in range(members):
        out[m, NECK_ROWS:] = parts


def finish(band_at, got, own_sixteen, own_thirty, table, eight, sixteen, thirty, sixty):
    members = got.shape[0]
    first = band_at[0] == 0
    neck = members * NECK_ROWS
    for r in range(members):
        source = jnp.where(first, r, members - 1 - r)
        eight[:, r * LANES : (r + 1) * LANES] = got[source, :NECK_ROWS]
    stats = jnp.sum(got[:, NECK_ROWS:].astype(F32), axis=0)
    stats = stats[:NECK_ROWS] + stats[NECK_ROWS : 2 * NECK_ROWS] + stats[2 * NECK_ROWS :]
    stats = stats / neck
    pieces = own_sixteen.shape[1] // LANES + 1

    def apply(values, k, index):
        gain, shift = scaled(table, index)
        center = stats[k : k + 1]
        spread = stats[pieces + k : pieces + k + 1] - center * center
        return ((values.astype(F32) - center) * lax.rsqrt(spread + EPSILON) * gain + shift).astype(BF)

    for k in range(pieces - 1):
        at = slice(k * LANES, (k + 1) * LANES)
        sixteen[:, at] = apply(own_sixteen[:, at], k, 3)
    last = apply(own_thirty[...], pieces - 1, 5)
    thirty[...] = last
    small = LANES // 4
    pick = one_hot(
        (LANES, sixty.shape[1]),
        lambda l: (l // (small // 2)) * (2 * small) + (l % (small // 2)) * 2,
    )
    sixty[...] = dot(last, pick).astype(BF)


def call(kernel, outs, where, *operands, scratch=(), space=pltpu.VMEM):
    specs = [pl.BlockSpec(memory_space=pltpu.SMEM) for _ in where] + [
        pl.BlockSpec(memory_space=space) for _ in operands
    ]
    return pl.pallas_call(
        kernel,
        in_specs=specs,
        out_specs=jax.tree.map(lambda _: pl.BlockSpec(memory_space=pltpu.VMEM), outs),
        out_shape=outs,
        scratch_shapes=scratch,
        compiler_params=pltpu.CompilerParams(vmem_limit_bytes=GRANT),
    )(*where, *(pltpu.with_memory_space_constraint(x, space) for x in operands))


def per_device(
    features,
    deconv_weight,
    deconv_bias,
    lateral_eight,
    lateral_coarse,
    output_conv,
    norm_gain,
    norm_shift,
):
    row_count, col_count, local = features.shape
    members = lax.axis_size(MP)
    pixels = row_count * col_count
    half_local = deconv_weight.shape[1]
    neck = norm_gain.shape[1]
    assert members == 2 * row_count and 2 * col_count == LANES
    assert lateral_eight.shape[0] == NECK_ROWS and members * NECK_ROWS == neck
    shape = jax.ShapeDtypeStruct
    band, row, plane = (
        lax.axis_index(axis).astype(jnp.int32).reshape(1) for axis in ("space", MP, "dp")
    )
    planes = lax.axis_size("dp")
    assert planes % SHARES == 0
    parity = plane & 1
    conv = output_conv.transpose(0, 2, 1, 3)
    share_rows = PER_SHARE * NECK_ROWS

    def from_plane(value, step):
        return lax.ppermute(value, "dp", [((i + step) % planes, i) for i in range(planes)])

    def from_core(value):
        return lax.ppermute(value, "space", [(0, 1), (1, 0)])

    blocks = call(
        spread_features,
        shape((members, local * pixels // LANES + share_rows, LANES), BF),
        (band, parity), features.reshape(pixels, local), conv, lateral_eight,
        space=pltpu.HBM,
        scratch=[
            pltpu.VMEM((pixels, local), BF),
            pltpu.VMEM(conv.shape[1:], BF),
            pltpu.VMEM(lateral_eight.shape, BF),
            pltpu.SemaphoreType.DMA((3,)),
        ],
    )
    gathered = lax.all_to_all(blocks, MP, 0, 0, tiled=True)
    blocks, share, share_low, share_high = call(
        raise_map,
        (
            shape((members, 3 * half_local + 5 * NECK_ROWS, LANES), BF),
            shape((members, share_rows, LANES), BF),
            shape((members // 2, share_rows, LANES), BF),
            shape((members // 2, share_rows, LANES), BF),
        ),
        (band,), gathered, deconv_weight, deconv_bias.reshape(1, half_local), lateral_coarse,
        scratch=[pltpu.VMEM((members, half_local, LANES), BF)],
    )
    got = lax.all_to_all(blocks, MP, 0, 0, tiled=True)
    share_low = from_plane(share_low, -1)
    share_high = from_plane(share_high, 1)
    mine = call(
        merge_shares,
        shape((SHARES, members, share_rows, LANES), BF),
        (parity,), share, share_low, share_high,
    )
    theirs = from_core(mine)
    got_other = from_core(got)
    total = call(
        level_eight,
        shape((neck, LANES), F32),
        (band, row), got, mine, theirs, norm_gain, norm_shift,
    )
    blocks, own_sixteen, own_thirty, table = call(
        levels,
        (
            shape((members, 4 * NECK_ROWS, LANES), BF),
            shape((NECK_ROWS, pixels), BF),
            shape((NECK_ROWS, pixels // 4), BF),
            shape((NECK_ROWS, 16), F32),
        ),
        (band, row), got, got_other, total, mine, theirs, conv, norm_gain, norm_shift,
        scratch=[pltpu.VMEM((neck, 16), F32)],
    )
    got = lax.all_to_all(blocks, MP, 0, 0, tiled=True)
    return call(
        finish,
        (
            shape((NECK_ROWS, 4 * pixels), BF),
            shape((NECK_ROWS, pixels), BF),
            shape((NECK_ROWS, pixels // 4), BF),
            shape((NECK_ROWS, pixels // 16), BF),
        ),
        (band,), got, own_sixteen, own_thirty, table,
    )


def solution(mesh):
    finer = Mesh(
        mesh.devices.reshape(mesh.shape["dp"], mesh.shape["space"], 4, 4),
        ("dp", "space", "mp_0", "mp_1"),
    )
    in_specs = (
        P(("dp", "space"), None, MP),
        P(None, MP, None),
        P(MP),
        P(MP, None),
        P(None, MP, None),
        P(None, MP, None, None),
        P(),
        P(),
    )
    return jax.shard_map(
        per_device,
        mesh=finer,
        in_specs=in_specs,
        out_specs=(P(MP, ("dp", "space")),) * 4,
        check_vma=False,
    )
```

```python
import jax
import jax.numpy as jnp
from jax import lax
from jax.experimental import pallas as pl
from jax.experimental.pallas import tpu as pltpu
from jax.sharding import Mesh
from jax.sharding import PartitionSpec as P


MP = ("mp_0", "mp_1")
EPSILON = 1e-06
BF = jnp.bfloat16
F32 = jnp.float32
LANES = 128
GRANT = 12 * 1024 * 1024
NECK_ROWS = 16
SHARES = 2
PER_SHARE = 6


GATHER_ORDER, SPREAD_ORDER, RETURN_ORDER = -1, 1, -1


def place(index, members, order):
    return index if order > 0 else members - 1 - index


def exchanged(blocks, order):
    members = blocks.shape[0]
    groups = [[place(m, members, order) for m in range(members)]]
    return lax.all_to_all(blocks, MP, 0, 0, tiled=True, axis_index_groups=None if order > 0 else groups)


def by_source(blocks, order):
    if order < 0:
        blocks = jnp.concatenate([blocks[m : m + 1] for m in reversed(range(blocks.shape[0]))], axis=0)
    return blocks


def dot(a, b):
    return jnp.dot(a, b, preferred_element_type=F32)


def iota(shape, dim):
    return lax.broadcasted_iota(jnp.int32, shape, dim)


def one_hot(shape, source_of_column):
    rows = iota(shape, 0)
    columns = iota(shape, 1)
    return jnp.where(rows == source_of_column(columns), 1.0, 0.0).astype(BF)


def channel_norm(values, gain, shift):
    count = values.shape[0]
    center = jnp.sum(values, axis=0, keepdims=True) / count
    spread = jnp.sum(values * values, axis=0, keepdims=True) / count - center * center
    return (values - center) * lax.rsqrt(spread + EPSILON) * gain + shift


def weight_piece(halves, index):
    share, at = index // PER_SHARE, index % PER_SHARE
    return jnp.concatenate(
        [
            half[share, :, at * NECK_ROWS : (at + 1) * NECK_ROWS].reshape(-1, LANES)
            for half in halves
        ],
        axis=1,
    )


def spread_features(
    band_at, parity_at, x_from, conv_from, lat_from, out, x, conv, lat, arrived
):
    copies = [
        pltpu.make_async_copy(x_from, x, arrived.at[0]),
        pltpu.make_async_copy(conv_from.at[0], conv, arrived.at[1]),
        pltpu.make_async_copy(lat_from, lat, arrived.at[2]),
    ]
    for copy in copies:
        copy.start()
    for copy in copies:
        copy.wait()
    members = out.shape[0]
    first = band_at[0] == 0
    even = parity_at[0] == 0
    flat = x[...].astype(F32).T.astype(BF)
    flat = jnp.concatenate(
        [flat[:, k : k + LANES] for k in range(0, flat.shape[1], LANES)], axis=0
    )
    half = lat.shape[1] // 2
    lateral = jnp.where(first, lat[:, :half], lat[:, half:])
    pieces = [jnp.where(first, conv[t, :, :LANES], conv[t, :, LANES:]) for t in range(9)]
    pieces += [lateral[:, :LANES], lateral[:, LANES:], lateral[:, LANES:]]
    weights = [jnp.where(even, pieces[k], pieces[PER_SHARE + k]) for k in range(PER_SHARE)]
    weights = jnp.concatenate(weights, axis=0)
    start = flat.shape[0]
    for m in range(members):
        out[m, :start] = flat
        out[m, start:] = weights


def raise_map(band_at, gathered, deconv, bias, coarse_w, out, share, share_low, share_high, rows):
    members = gathered.shape[0]
    taps, half_local, depth = deconv.shape
    local = depth // members
    weight_rows = share.shape[1]
    split = gathered.shape[1] - weight_rows
    pixels = split // local * LANES
    half = members // 2
    weights = by_source(gathered[:, split:], GATHER_ORDER)
    share[...] = weights
    share_low[...] = weights[:half]
    share_high[...] = weights[half:]
    x = jnp.concatenate(
        [
            by_source(gathered[:, k : k + local], GATHER_ORDER).reshape(depth, LANES)
            for k in range(0, split, local)
        ],
        axis=1,
    )
    columns = 2 * pixels // members
    raised = dot(deconv[...].reshape(taps * half_local, depth), x)
    diagonal = iota((half_local, half_local), 0) == iota((half_local, half_local), 1)
    bias_column = jnp.sum(jnp.where(diagonal, bias[...], 0.0), axis=1, keepdims=True)
    low = iota((half_local, LANES), 1) < columns
    for a in range(2):
        for p in range(pixels // LANES):
            tiles = [
                raised[
                    (2 * a + b) * half_local : (2 * a + b + 1) * half_local,
                    p * LANES : (p + 1) * LANES,
                ]
                + bias_column
                for b in range(2)
            ]
            swapped = [pltpu.roll(tile, columns, 1) for tile in tiles]
            rows[4 * p + a] = jnp.where(low, tiles[0], swapped[1]).astype(BF)
            rows[4 * p + 2 + a] = jnp.where(low, swapped[0], tiles[1]).astype(BF)
    middle = dot(coarse_w[0], x).astype(BF)
    low = iota((depth, LANES), 1) < columns
    pairs = []
    for p in range(pixels // LANES):
        tile = x[:, p * LANES : (p + 1) * LANES].astype(F32)
        pairs.append(jnp.maximum(tile, pltpu.roll(tile, columns, 1)))
    packed = []
    for p in range(0, len(pairs), 2):
        both = jnp.where(low, pairs[p], pairs[p + 1])
        packed.append(jnp.maximum(both, pltpu.roll(both, LANES - 1, 1)).astype(BF))
    coarse = dot(coarse_w[1], jnp.concatenate(packed, axis=1)).astype(BF)
    coarse = dot(coarse, one_hot((pixels // 2, LANES), lambda l: 2 * l)).astype(BF)
    tail = [middle[:, p * LANES : (p + 1) * LANES] for p in range(pixels // LANES)] + [coarse]
    tail = jnp.concatenate(tail, axis=0)
    first = band_at[0] == 0
    for m in range(members):
        row = jnp.where(first, m, members - 1 - m)
        at = place(m, members, SPREAD_ORDER)
        for k in range(3):
            out[at, k * half_local : (k + 1) * half_local] = rows[
                jnp.clip(row + k - 1, 0, members - 1)
            ]
        out[at, 3 * half_local :] = tail


def columns_of(gain, shift):
    blank = jnp.zeros((2, gain.shape[1]), F32)
    return jnp.concatenate([gain[...], blank, shift[...], blank], axis=0).T


def scaled(table, index):
    return table[:, index : index + 1], table[:, 8 + index : 9 + index]


def merge_shares(parity_at, own, low, high, out):
    parity = parity_at[0]
    middle = low.shape[0]
    out[parity] = own[...]
    out[1 - parity, :middle] = low[...]
    out[1 - parity, middle:] = high[...]


def lateral_weight(halves):
    pair = [weight_piece([half], 9 + k) for half in halves for k in range(2)]
    return jnp.concatenate(pair, axis=1)


def windows(center):
    lane = iota(center.shape, 1)
    columns = LANES // 2
    odd = lane >= columns
    swapped = pltpu.roll(center, columns, 1)
    left = jnp.where(odd, swapped, pltpu.roll(swapped, 1, 1))
    left = jnp.where(lane == 0, 0.0, left)
    right = jnp.where(odd, pltpu.roll(swapped, LANES - 1, 1), swapped)
    right = jnp.where(lane == LANES - 1, 0.0, right)
    return [window.astype(BF) for window in (left, center, right)]


def ordered_halves(first, mine, theirs):
    low = jnp.where(first, mine[...], theirs[...])
    high = jnp.where(first, theirs[...], mine[...])
    return low, high


def level_eight(band_at, row_at, got, mine, theirs, gain, shift, total_out):
    members = got.shape[0]
    first = band_at[0] == 0
    row = jnp.where(first, row_at[0], members - 1 - row_at[0])
    half_local = (got.shape[1] - 5 * NECK_ROWS) // 3
    table = columns_of(gain, shift)
    halves = ordered_halves(first, mine, theirs)
    raised = jnp.concatenate(
        [
            by_source(got[:, r * half_local : (r + 1) * half_local], SPREAD_ORDER).reshape(
                members * half_local, LANES
            )
            for r in range(3)
        ],
        axis=1,
    )
    lat = dot(lateral_weight(halves), raised).astype(BF).astype(F32)
    normed = channel_norm(lat, *scaled(table, 0))
    total = None
    for r in range(3):
        center = normed[:, r * LANES : (r + 1) * LANES]
        if r == 0:
            center = jnp.where(row == 0, 0.0, center)
        if r == 2:
            center = jnp.where(row == members - 1, 0.0, center)
        for q, window in enumerate(windows(center)):
            part = dot(weight_piece(halves, 3 * r + q), window)
            total = part if total is None else total + part
    total_out[...] = total


def small_conv(normed, halo, weight, width, first):
    taps, out_local, depth = weight.shape
    stacked = weight.reshape(taps * out_local, depth)
    main = dot(stacked, normed)
    rim = dot(stacked, halo)
    cells = normed.shape[1]

    def across(values, r):
        size = values.shape[1]
        column = iota((out_local, size), 1) % width
        pieces = [
            values[(3 * r + q) * out_local : (3 * r + q + 1) * out_local] for q in range(3)
        ]
        left = jnp.where(column == 0, 0.0, pltpu.roll(pieces[0], 1, 1))
        right = jnp.where(column == width - 1, 0.0, pltpu.roll(pieces[2], size - 1, 1))
        return left + pieces[1] + right

    lane = iota((out_local, cells), 1)
    rim_above = jnp.where(first, 0.0, across(rim, 0))
    rim_below = jnp.where(first, pltpu.roll(across(rim, 2), LANES - width, 1), 0.0)
    if cells > LANES:
        blank = jnp.zeros((out_local, cells - LANES), F32)
        rim_above = jnp.concatenate([rim_above, blank], axis=1)
        rim_below = jnp.concatenate([blank, rim_below], axis=1)
    above = jnp.where(lane < width, rim_above, pltpu.roll(across(main, 0), width, 1))
    below = jnp.where(
        lane >= cells - width, rim_below, pltpu.roll(across(main, 2), cells - width, 1)
    )
    return above + across(main, 1) + below


def levels(
    band_at, row_at, got, got_other, total, mine, theirs, conv, gain, shift,
    out, own_sixteen, own_thirty, own_table, table_at,
):
    members = got.shape[0]
    first = band_at[0] == 0
    neck = members * NECK_ROWS
    half_local = (got.shape[1] - 5 * NECK_ROWS) // 3
    columns = LANES // 2
    table = columns_of(gain, shift)
    table_at[...] = table
    start = pl.multiple_of(row_at[0] * NECK_ROWS, NECK_ROWS)
    own_table[...] = table_at[pl.ds(start, NECK_ROWS), :]

    halves = ordered_halves(first, mine, theirs)
    raised = by_source(got_other[:, half_local : 2 * half_local], SPREAD_ORDER)
    raised = raised.reshape(members * half_local, LANES)
    lat = dot(lateral_weight(halves), raised).astype(BF).astype(F32)
    center = channel_norm(lat, *scaled(table, 0))
    center = jnp.where(row_at[0] == members - 1, center, 0.0)
    convolved = total[...]
    for q, window in enumerate(windows(center)):
        tap = jnp.where(first, weight_piece(halves, 6 + q), weight_piece(halves, q))
        convolved = convolved + dot(tap, window)
    convolved = convolved.astype(BF).astype(F32)
    level = channel_norm(convolved, *scaled(table, 1)).astype(BF)
    mix = one_hot((LANES, LANES), lambda l: (l % 2) * columns + l // 2)
    level = dot(level, mix).astype(BF).reshape(members, NECK_ROWS, LANES)
    for m in range(members):
        out[place(m, members, RETURN_ORDER), :NECK_ROWS] = level[m]

    def tile(source, k):
        base = 3 * half_local + k * NECK_ROWS
        return by_source(source[:, base : base + NECK_ROWS], SPREAD_ORDER).reshape(neck, LANES).astype(F32)

    middle = jnp.concatenate([tile(got, k) for k in range(4)], axis=1)
    rim = jnp.where(first, tile(got_other, 0), pltpu.roll(tile(got_other, 3), columns, 1))
    sixteen = small_conv(
        channel_norm(middle, *scaled(table, 2)).astype(BF),
        channel_norm(rim, *scaled(table, 2)).astype(BF),
        conv[1], columns, first,
    ).astype(BF)
    rim = tile(got_other, 4)
    rim = jnp.where(first, rim, pltpu.roll(rim, columns // 2, 1))
    thirty = small_conv(
        channel_norm(tile(got, 4), *scaled(table, 4)).astype(BF),
        channel_norm(rim, *scaled(table, 4)).astype(BF),
        conv[2], columns // 2, first,
    ).astype(BF)
    own_sixteen[...] = sixteen
    own_thirty[...] = thirty
    floats = jnp.concatenate([sixteen, thirty], axis=1).astype(F32)
    sums = jnp.sum(floats, axis=0, keepdims=True)
    squares = jnp.sum(floats * floats, axis=0, keepdims=True)
    pieces = floats.shape[1] // LANES
    stats = jnp.concatenate(
        [part[:, k * LANES : (k + 1) * LANES] for part in (sums, squares) for k in range(pieces)]
        + [jnp.zeros((NECK_ROWS - 2 * pieces, LANES), F32)],
        axis=0,
    )
    parts = []
    for _ in range(3):
        parts.append(stats.astype(BF))
        stats = stats - parts[-1].astype(F32)
    parts = jnp.concatenate(parts, axis=0)
    for m in range(members):
        out[m, NECK_ROWS:] = parts


def finish(band_at, got, own_sixteen, own_thirty, table, eight, sixteen, thirty, sixty):
    members = got.shape[0]
    first = band_at[0] == 0
    neck = members * NECK_ROWS
    for r in range(members):
        source = jnp.where(first == (RETURN_ORDER > 0), r, members - 1 - r)
        eight[:, r * LANES : (r + 1) * LANES] = got[source, :NECK_ROWS]
    stats = jnp.sum(got[:, NECK_ROWS:].astype(F32), axis=0)
    stats = stats[:NECK_ROWS] + stats[NECK_ROWS : 2 * NECK_ROWS] + stats[2 * NECK_ROWS :]
    stats = stats / neck
    pieces = own_sixteen.shape[1] // LANES + 1

    def apply(values, k, index):
        gain, shift = scaled(table, index)
        center = stats[k : k + 1]
        spread = stats[pieces + k : pieces + k + 1] - center * center
        return ((values.astype(F32) - center) * lax.rsqrt(spread + EPSILON) * gain + shift).astype(BF)

    for k in range(pieces - 1):
        at = slice(k * LANES, (k + 1) * LANES)
        sixteen[:, at] = apply(own_sixteen[:, at], k, 3)
    last = apply(own_thirty[...], pieces - 1, 5)
    thirty[...] = last
    small = LANES // 4
    pick = one_hot(
        (LANES, sixty.shape[1]),
        lambda l: (l // (small // 2)) * (2 * small) + (l % (small // 2)) * 2,
    )
    sixty[...] = dot(last, pick).astype(BF)


def call(kernel, outs, where, *operands, scratch=(), space=pltpu.VMEM):
    specs = [pl.BlockSpec(memory_space=pltpu.SMEM) for _ in where] + [
        pl.BlockSpec(memory_space=space) for _ in operands
    ]
    return pl.pallas_call(
        kernel,
        in_specs=specs,
        out_specs=jax.tree.map(lambda _: pl.BlockSpec(memory_space=pltpu.VMEM), outs),
        out_shape=outs,
        scratch_shapes=scratch,
        compiler_params=pltpu.CompilerParams(vmem_limit_bytes=GRANT),
    )(*where, *(pltpu.with_memory_space_constraint(x, space) for x in operands))


def per_device(
    features,
    deconv_weight,
    deconv_bias,
    lateral_eight,
    lateral_coarse,
    output_conv,
    norm_gain,
    norm_shift,
):
    row_count, col_count, local = features.shape
    members = lax.axis_size(MP)
    pixels = row_count * col_count
    half_local = deconv_weight.shape[1]
    neck = norm_gain.shape[1]
    assert members == 2 * row_count and 2 * col_count == LANES
    assert lateral_eight.shape[0] == NECK_ROWS and members * NECK_ROWS == neck
    shape = jax.ShapeDtypeStruct
    band, row, plane = (
        lax.axis_index(axis).astype(jnp.int32).reshape(1) for axis in ("space", MP, "dp")
    )
    planes = lax.axis_size("dp")
    assert planes % SHARES == 0
    parity = plane & 1
    conv = output_conv.transpose(0, 2, 1, 3)
    share_rows = PER_SHARE * NECK_ROWS

    def from_plane(value, step):
        return lax.ppermute(value, "dp", [((i + step) % planes, i) for i in range(planes)])

    def from_core(value):
        return lax.ppermute(value, "space", [(0, 1), (1, 0)])

    blocks = call(
        spread_features,
        shape((members, local * pixels // LANES + share_rows, LANES), BF),
        (band, parity), features.reshape(pixels, local), conv, lateral_eight,
        space=pltpu.HBM,
        scratch=[
            pltpu.VMEM((pixels, local), BF),
            pltpu.VMEM(conv.shape[1:], BF),
            pltpu.VMEM(lateral_eight.shape, BF),
            pltpu.SemaphoreType.DMA((3,)),
        ],
    )
    gathered = exchanged(blocks, GATHER_ORDER)
    blocks, share, share_low, share_high = call(
        raise_map,
        (
            shape((members, 3 * half_local + 5 * NECK_ROWS, LANES), BF),
            shape((members, share_rows, LANES), BF),
            shape((members // 2, share_rows, LANES), BF),
            shape((members // 2, share_rows, LANES), BF),
        ),
        (band,), gathered, deconv_weight, deconv_bias.reshape(1, half_local), lateral_coarse,
        scratch=[pltpu.VMEM((members, half_local, LANES), BF)],
    )
    got = exchanged(blocks, SPREAD_ORDER)
    share_low = from_plane(share_low, -1)
    share_high = from_plane(share_high, 1)
    mine = call(
        merge_shares,
        shape((SHARES, members, share_rows, LANES), BF),
        (parity,), share, share_low, share_high,
    )
    theirs = from_core(mine)
    got_other = from_core(got)
    total = call(
        level_eight,
        shape((neck, LANES), F32),
        (band, row), got, mine, theirs, norm_gain, norm_shift,
    )
    blocks, own_sixteen, own_thirty, table = call(
        levels,
        (
            shape((members, 4 * NECK_ROWS, LANES), BF),
            shape((NECK_ROWS, pixels), BF),
            shape((NECK_ROWS, pixels // 4), BF),
            shape((NECK_ROWS, 16), F32),
        ),
        (band, row), got, got_other, total, mine, theirs, conv, norm_gain, norm_shift,
        scratch=[pltpu.VMEM((neck, 16), F32)],
    )
    got = exchanged(blocks, RETURN_ORDER)
    return call(
        finish,
        (
            shape((NECK_ROWS, 4 * pixels), BF),
            shape((NECK_ROWS, pixels), BF),
            shape((NECK_ROWS, pixels // 4), BF),
            shape((NECK_ROWS, pixels // 16), BF),
        ),
        (band,), got, own_sixteen, own_thirty, table,
    )


def solution(mesh):
    finer = Mesh(
        mesh.devices.reshape(mesh.shape["dp"], mesh.shape["space"], 4, 4),
        ("dp", "space", "mp_0", "mp_1"),
    )
    in_specs = (
        P(("dp", "space"), None, MP),
        P(None, MP, None),
        P(MP),
        P(MP, None),
        P(None, MP, None),
        P(None, MP, None, None),
        P(),
        P(),
    )
    return jax.shard_map(
        per_device,
        mesh=finer,
        in_specs=in_specs,
        out_specs=(P(MP, ("dp", "space")),) * 4,
        check_vma=False,
    )
```

```python
import jax
import jax.numpy as jnp
from jax import lax
from jax.experimental import pallas as pl
from jax.experimental.pallas import tpu as pltpu
from jax.sharding import Mesh
from jax.sharding import PartitionSpec as P


MP = ("mp_0", "mp_1")
EPSILON = 1e-06
BF = jnp.bfloat16
F32 = jnp.float32
LANES = 128
GRANT = 12 * 1024 * 1024
NECK_ROWS = 16
SHARES = 2
PER_SHARE = 6


MEMBERS = 16
GATHER_ORDER = tuple((m + 10) % MEMBERS for m in range(MEMBERS))
SPREAD_ORDER = tuple(range(MEMBERS))
RETURN_ORDER = tuple((m + 10) % MEMBERS for m in range(MEMBERS))


def place(index, order):
    return order.index(index)


def exchanged(blocks, order):
    return lax.all_to_all(blocks, MP, 0, 0, tiled=True, axis_index_groups=[list(order)])


def by_source(blocks, order):
    places = [place(m, order) for m in range(MEMBERS)]
    return jnp.concatenate([blocks[k : k + 1] for k in places], axis=0)


def dot(a, b):
    return jnp.dot(a, b, preferred_element_type=F32)


def iota(shape, dim):
    return lax.broadcasted_iota(jnp.int32, shape, dim)


def one_hot(shape, source_of_column):
    rows = iota(shape, 0)
    columns = iota(shape, 1)
    return jnp.where(rows == source_of_column(columns), 1.0, 0.0).astype(BF)


def channel_norm(values, gain, shift):
    count = values.shape[0]
    center = jnp.sum(values, axis=0, keepdims=True) / count
    spread = jnp.sum(values * values, axis=0, keepdims=True) / count - center * center
    return (values - center) * lax.rsqrt(spread + EPSILON) * gain + shift


def weight_piece(halves, index):
    share, at = index // PER_SHARE, index % PER_SHARE
    return jnp.concatenate(
        [
            half[share][:, at * NECK_ROWS : (at + 1) * NECK_ROWS].reshape(-1, LANES)
            for half in halves
        ],
        axis=1,
    )


def spread_features(
    band_at, parity_at, x_from, conv_from, lat_from, out, x, conv, lat, arrived
):
    copies = [
        pltpu.make_async_copy(x_from, x, arrived.at[0]),
        pltpu.make_async_copy(conv_from.at[0], conv, arrived.at[1]),
        pltpu.make_async_copy(lat_from, lat, arrived.at[2]),
    ]
    for copy in copies:
        copy.start()
    for copy in copies:
        copy.wait()
    members = out.shape[0]
    first = band_at[0] == 0
    even = parity_at[0] == 0
    flat = x[...].astype(F32).T.astype(BF)
    flat = jnp.concatenate(
        [flat[:, k : k + LANES] for k in range(0, flat.shape[1], LANES)], axis=0
    )
    half = lat.shape[1] // 2
    lateral = jnp.where(first, lat[:, :half], lat[:, half:])
    pieces = [jnp.where(first, conv[t, :, :LANES], conv[t, :, LANES:]) for t in range(9)]
    pieces += [lateral[:, :LANES], lateral[:, LANES:], lateral[:, LANES:]]
    weights = [jnp.where(even, pieces[k], pieces[PER_SHARE + k]) for k in range(PER_SHARE)]
    weights = jnp.concatenate(weights, axis=0)
    start = flat.shape[0]
    for m in range(members):
        out[m, :start] = flat
        out[m, start:] = weights


def raise_map(band_at, gathered, deconv, bias, coarse_w, out, share, share_low, share_high, rows):
    members = gathered.shape[0]
    taps, half_local, depth = deconv.shape
    local = depth // members
    weight_rows = share.shape[1]
    split = gathered.shape[1] - weight_rows
    pixels = split // local * LANES
    half = members // 2
    weights = by_source(gathered[:, split:], GATHER_ORDER)
    share[...] = weights
    share_low[...] = weights[:half]
    share_high[...] = weights[half:]
    x = jnp.concatenate(
        [
            by_source(gathered[:, k : k + local], GATHER_ORDER).reshape(depth, LANES)
            for k in range(0, split, local)
        ],
        axis=1,
    )
    columns = 2 * pixels // members
    raised = dot(deconv[...].reshape(taps * half_local, depth), x)
    diagonal = iota((half_local, half_local), 0) == iota((half_local, half_local), 1)
    bias_column = jnp.sum(jnp.where(diagonal, bias[...], 0.0), axis=1, keepdims=True)
    low = iota((half_local, LANES), 1) < columns
    for a in range(2):
        for p in range(pixels // LANES):
            tiles = [
                raised[
                    (2 * a + b) * half_local : (2 * a + b + 1) * half_local,
                    p * LANES : (p + 1) * LANES,
                ]
                + bias_column
                for b in range(2)
            ]
            swapped = [pltpu.roll(tile, columns, 1) for tile in tiles]
            rows[4 * p + a] = jnp.where(low, tiles[0], swapped[1]).astype(BF)
            rows[4 * p + 2 + a] = jnp.where(low, swapped[0], tiles[1]).astype(BF)
    middle = dot(coarse_w[0], x).astype(BF)
    low = iota((depth, LANES), 1) < columns
    pairs = []
    for p in range(pixels // LANES):
        tile = x[:, p * LANES : (p + 1) * LANES].astype(F32)
        pairs.append(jnp.maximum(tile, pltpu.roll(tile, columns, 1)))
    packed = []
    for p in range(0, len(pairs), 2):
        both = jnp.where(low, pairs[p], pairs[p + 1])
        packed.append(jnp.maximum(both, pltpu.roll(both, LANES - 1, 1)).astype(BF))
    coarse = dot(coarse_w[1], jnp.concatenate(packed, axis=1)).astype(BF)
    coarse = dot(coarse, one_hot((pixels // 2, LANES), lambda l: 2 * l)).astype(BF)
    tail = [middle[:, p * LANES : (p + 1) * LANES] for p in range(pixels // LANES)] + [coarse]
    tail = jnp.concatenate(tail, axis=0)
    first = band_at[0] == 0
    for m in range(members):
        row = jnp.where(first, m, members - 1 - m)
        at = place(m, SPREAD_ORDER)
        for k in range(3):
            out[at, k * half_local : (k + 1) * half_local] = rows[
                jnp.clip(row + k - 1, 0, members - 1)
            ]
        out[at, 3 * half_local :] = tail


def columns_of(gain, shift):
    blank = jnp.zeros((2, gain.shape[1]), F32)
    return jnp.concatenate([gain[...], blank, shift[...], blank], axis=0).T


def scaled(table, index):
    return table[:, index : index + 1], table[:, 8 + index : 9 + index]


def merge_shares(parity_at, own, low, high, out):
    parity = parity_at[0]
    middle = low.shape[0]
    out[parity] = own[...]
    out[1 - parity, :middle] = low[...]
    out[1 - parity, middle:] = high[...]


def lateral_weight(halves):
    pair = [weight_piece([half], 9 + k) for half in halves for k in range(2)]
    return jnp.concatenate(pair, axis=1)


def windows(center):
    lane = iota(center.shape, 1)
    columns = LANES // 2
    odd = lane >= columns
    swapped = pltpu.roll(center, columns, 1)
    left = jnp.where(odd, swapped, pltpu.roll(swapped, 1, 1))
    left = jnp.where(lane == 0, 0.0, left)
    right = jnp.where(odd, pltpu.roll(swapped, LANES - 1, 1), swapped)
    right = jnp.where(lane == LANES - 1, 0.0, right)
    return [window.astype(BF) for window in (left, center, right)]


def ordered_halves(first, mine, theirs):
    low = jnp.where(first, mine[...], theirs[...])
    high = jnp.where(first, theirs[...], mine[...])
    return low, high


def lateral_tile(source, k, start):
    base = start + k * NECK_ROWS
    rows = by_source(source[:, base : base + NECK_ROWS], SPREAD_ORDER)
    return rows.reshape(-1, LANES).astype(F32)


def own_band(
    band_at, row_at, got, mine, theirs, conv, gain, shift,
    total_out, sixteen_out, thirty_out,
):
    members = got.shape[0]
    first = band_at[0] == 0
    row = jnp.where(first, row_at[0], members - 1 - row_at[0])
    half_local = (got.shape[1] - 5 * NECK_ROWS) // 3
    table = columns_of(gain, shift)
    halves = ordered_halves(first, mine, theirs)
    raised = jnp.concatenate(
        [
            by_source(got[:, r * half_local : (r + 1) * half_local], SPREAD_ORDER).reshape(
                members * half_local, LANES
            )
            for r in range(3)
        ],
        axis=1,
    )
    lat = dot(lateral_weight(halves), raised).astype(BF).astype(F32)
    normed = channel_norm(lat, *scaled(table, 0))
    total = None
    for r in range(3):
        center = normed[:, r * LANES : (r + 1) * LANES]
        if r == 0:
            center = jnp.where(row == 0, 0.0, center)
        if r == 2:
            center = jnp.where(row == members - 1, 0.0, center)
        for q, window in enumerate(windows(center)):
            part = dot(weight_piece(halves, 3 * r + q), window)
            total = part if total is None else total + part
    total_out[...] = total
    start = 3 * half_local
    middle = jnp.concatenate([lateral_tile(got, k, start) for k in range(4)], axis=1)
    normed = channel_norm(middle, *scaled(table, 2)).astype(BF)
    sixteen_out[...] = small_conv(normed, conv[1], LANES // 2)
    normed = channel_norm(lateral_tile(got, 4, start), *scaled(table, 4)).astype(BF)
    thirty_out[...] = small_conv(normed, conv[2], LANES // 4)


def across(products, r, out_local, width):
    size = products.shape[1]
    column = iota((out_local, size), 1) % width
    pieces = [
        products[(3 * r + q) * out_local : (3 * r + q + 1) * out_local] for q in range(3)
    ]
    left = jnp.where(column == 0, 0.0, pltpu.roll(pieces[0], 1, 1))
    right = jnp.where(column == width - 1, 0.0, pltpu.roll(pieces[2], size - 1, 1))
    return left + pieces[1] + right


def small_conv(normed, weight, width):
    taps, out_local, depth = weight.shape
    products = dot(weight.reshape(taps * out_local, depth), normed)
    cells = normed.shape[1]
    lane = iota((out_local, cells), 1)
    above = pltpu.roll(across(products, 0, out_local, width), width, 1)
    below = pltpu.roll(across(products, 2, out_local, width), cells - width, 1)
    above = jnp.where(lane < width, 0.0, above)
    below = jnp.where(lane >= cells - width, 0.0, below)
    return above + across(products, 1, out_local, width) + below


def small_rim(total, halo, weight, width, first):
    taps, out_local, depth = weight.shape
    products = dot(weight.reshape(taps * out_local, depth), halo)
    cells = total.shape[1]
    lane = iota((out_local, LANES), 1)
    above = jnp.where(lane < width, across(products, 0, out_local, width), 0.0)
    below = jnp.where(lane < width, across(products, 2, out_local, width), 0.0)
    above = jnp.where(first, 0.0, above)
    below = jnp.where(first, pltpu.roll(below, LANES - width, 1), 0.0)
    if cells == LANES:
        return total + (above + below)
    return jnp.concatenate(
        [total[:, :LANES] + above, total[:, LANES : cells - LANES], total[:, cells - LANES :] + below],
        axis=1,
    )


def levels(
    band_at, row_at, got_other, total, total_sixteen, total_thirty, mine, theirs, conv, gain, shift,
    out, own_sixteen, own_thirty, own_table, table_at,
):
    members = got_other.shape[0]
    first = band_at[0] == 0
    half_local = (got_other.shape[1] - 5 * NECK_ROWS) // 3
    columns = LANES // 2
    table = columns_of(gain, shift)
    table_at[...] = table
    start = pl.multiple_of(row_at[0] * NECK_ROWS, NECK_ROWS)
    own_table[...] = table_at[pl.ds(start, NECK_ROWS), :]

    halves = ordered_halves(first, mine, theirs)
    raised = by_source(got_other[:, half_local : 2 * half_local], SPREAD_ORDER)
    raised = raised.reshape(members * half_local, LANES)
    lat = dot(lateral_weight(halves), raised).astype(BF).astype(F32)
    center = channel_norm(lat, *scaled(table, 0))
    center = jnp.where(row_at[0] == members - 1, center, 0.0)
    convolved = total[...]
    for q, window in enumerate(windows(center)):
        tap = jnp.where(first, weight_piece(halves, 6 + q), weight_piece(halves, q))
        convolved = convolved + dot(tap, window)
    convolved = convolved.astype(BF).astype(F32)
    level = channel_norm(convolved, *scaled(table, 1)).astype(BF)
    mix = one_hot((LANES, LANES), lambda l: (l % 2) * columns + l // 2)
    level = dot(level, mix).astype(BF).reshape(members, NECK_ROWS, LANES)
    for m in range(members):
        out[place(m, RETURN_ORDER), :NECK_ROWS] = level[m]

    start = 3 * half_local
    rim = lateral_tile(got_other, 3, start)
    rim = jnp.where(first, lateral_tile(got_other, 0, start), pltpu.roll(rim, columns, 1))
    normed = channel_norm(rim, *scaled(table, 2)).astype(BF)
    sixteen = small_rim(total_sixteen[...], normed, conv[1], columns, first).astype(BF)
    rim = lateral_tile(got_other, 4, start)
    rim = jnp.where(first, rim, pltpu.roll(rim, columns // 2, 1))
    normed = channel_norm(rim, *scaled(table, 4)).astype(BF)
    thirty = small_rim(total_thirty[...], normed, conv[2], columns // 2, first).astype(BF)
    own_sixteen[...] = sixteen
    own_thirty[...] = thirty
    floats = jnp.concatenate([sixteen, thirty], axis=1).astype(F32)
    sums = jnp.sum(floats, axis=0, keepdims=True)
    squares = jnp.sum(floats * floats, axis=0, keepdims=True)
    pieces = floats.shape[1] // LANES
    stats = jnp.concatenate(
        [part[:, k * LANES : (k + 1) * LANES] for part in (sums, squares) for k in range(pieces)]
        ,
        axis=0,
    )
    parts = []
    for _ in range(3):
        parts.append(stats.astype(BF))
        stats = stats - parts[-1].astype(F32)
    parts.append(jnp.zeros((out.shape[1] - NECK_ROWS - 6 * pieces, LANES), BF))
    parts = jnp.concatenate([part.astype(F32) for part in parts], axis=0).astype(BF)
    for m in range(members):
        out[m, NECK_ROWS:] = parts


def finish(band_at, got, own_sixteen, own_thirty, table, eight, sixteen, thirty, sixty):
    members = got.shape[0]
    first = band_at[0] == 0
    neck = members * NECK_ROWS
    for r in range(members):
        source = jnp.where(
            first, place(r, RETURN_ORDER), place(members - 1 - r, RETURN_ORDER)
        )
        eight[:, r * LANES : (r + 1) * LANES] = got[source, :NECK_ROWS]
    stats = jnp.sum(got[:, NECK_ROWS:].astype(F32), axis=0)
    pieces = own_sixteen.shape[1] // LANES + 1
    stats = sum(stats[2 * pieces * k : 2 * pieces * (k + 1)] for k in range(3)) / neck

    def apply(values, k, index):
        gain, shift = scaled(table, index)
        center = stats[k : k + 1]
        spread = stats[pieces + k : pieces + k + 1] - center * center
        return ((values.astype(F32) - center) * lax.rsqrt(spread + EPSILON) * gain + shift).astype(BF)

    for k in range(pieces - 1):
        at = slice(k * LANES, (k + 1) * LANES)
        sixteen[:, at] = apply(own_sixteen[:, at], k, 3)
    last = apply(own_thirty[...], pieces - 1, 5)
    thirty[...] = last
    small = LANES // 4
    pick = one_hot(
        (LANES, sixty.shape[1]),
        lambda l: (l // (small // 2)) * (2 * small) + (l % (small // 2)) * 2,
    )
    sixty[...] = dot(last, pick).astype(BF)


def call(kernel, outs, where, *operands, scratch=(), space=pltpu.VMEM):
    specs = [pl.BlockSpec(memory_space=pltpu.SMEM) for _ in where] + [
        pl.BlockSpec(memory_space=space) for _ in operands
    ]
    return pl.pallas_call(
        kernel,
        in_specs=specs,
        out_specs=jax.tree.map(lambda _: pl.BlockSpec(memory_space=pltpu.VMEM), outs),
        out_shape=outs,
        scratch_shapes=scratch,
        compiler_params=pltpu.CompilerParams(vmem_limit_bytes=GRANT),
    )(*where, *(pltpu.with_memory_space_constraint(x, space) for x in operands))


def per_device(
    features,
    deconv_weight,
    deconv_bias,
    lateral_eight,
    lateral_coarse,
    output_conv,
    norm_gain,
    norm_shift,
):
    row_count, col_count, local = features.shape
    members = lax.axis_size(MP)
    pixels = row_count * col_count
    half_local = deconv_weight.shape[1]
    neck = norm_gain.shape[1]
    assert members == MEMBERS == 2 * row_count and 2 * col_count == LANES
    assert lateral_eight.shape[0] == NECK_ROWS and members * NECK_ROWS == neck
    shape = jax.ShapeDtypeStruct
    band, row, plane = (
        lax.axis_index(axis).astype(jnp.int32).reshape(1) for axis in ("space", MP, "dp")
    )
    planes = lax.axis_size("dp")
    assert planes % SHARES == 0
    parity = plane & 1
    conv = output_conv.transpose(0, 2, 1, 3)
    share_rows = PER_SHARE * NECK_ROWS

    def from_plane(value, step):
        return lax.ppermute(value, "dp", [((i + step) % planes, i) for i in range(planes)])

    def from_core(value):
        return lax.ppermute(value, "space", [(0, 1), (1, 0)])

    blocks = call(
        spread_features,
        shape((members, local * pixels // LANES + share_rows, LANES), BF),
        (band, parity), features.reshape(pixels, local), conv, lateral_eight,
        space=pltpu.HBM,
        scratch=[
            pltpu.VMEM((pixels, local), BF),
            pltpu.VMEM(conv.shape[1:], BF),
            pltpu.VMEM(lateral_eight.shape, BF),
            pltpu.SemaphoreType.DMA((3,)),
        ],
    )
    gathered = exchanged(blocks, GATHER_ORDER)
    blocks, share, share_low, share_high = call(
        raise_map,
        (
            shape((members, 3 * half_local + 5 * NECK_ROWS, LANES), BF),
            shape((members, share_rows, LANES), BF),
            shape((members // 2, share_rows, LANES), BF),
            shape((members // 2, share_rows, LANES), BF),
        ),
        (band,), gathered, deconv_weight, deconv_bias.reshape(1, half_local), lateral_coarse,
        scratch=[pltpu.VMEM((members, half_local, LANES), BF)],
    )
    got = exchanged(blocks, SPREAD_ORDER)
    share_low = from_plane(share_low, -1)
    share_high = from_plane(share_high, 1)
    mine = call(
        merge_shares,
        shape((SHARES, members, share_rows, LANES), BF),
        (parity,), share, share_low, share_high,
    )
    theirs = from_core(mine)
    got_other = from_core(got)
    where = (band, row)
    weights = (mine, theirs)
    total, total_sixteen, total_thirty = call(
        own_band,
        (
            shape((neck, LANES), F32),
            shape((NECK_ROWS, pixels), F32),
            shape((NECK_ROWS, pixels // 4), F32),
        ),
        where, got, *weights, conv, norm_gain, norm_shift,
    )
    blocks, own_sixteen, own_thirty, table = call(
        levels,
        (
            shape((members, 3 * NECK_ROWS, LANES), BF),
            shape((NECK_ROWS, pixels), BF),
            shape((NECK_ROWS, pixels // 4), BF),
            shape((NECK_ROWS, 16), F32),
        ),
        where, got_other, total, total_sixteen, total_thirty, *weights, conv, norm_gain, norm_shift,
        scratch=[pltpu.VMEM((neck, 16), F32)],
    )
    got = exchanged(blocks, RETURN_ORDER)
    return call(
        finish,
        (
            shape((NECK_ROWS, 4 * pixels), BF),
            shape((NECK_ROWS, pixels), BF),
            shape((NECK_ROWS, pixels // 4), BF),
            shape((NECK_ROWS, pixels // 16), BF),
        ),
        (band,), got, own_sixteen, own_thirty, table,
    )


def solution(mesh):
    finer = Mesh(
        mesh.devices.reshape(mesh.shape["dp"], mesh.shape["space"], 4, 4),
        ("dp", "space", "mp_0", "mp_1"),
    )
    in_specs = (
        P(("dp", "space"), None, MP),
        P(None, MP, None),
        P(MP),
        P(MP, None),
        P(None, MP, None),
        P(None, MP, None, None),
        P(),
        P(),
    )
    return jax.shard_map(
        per_device,
        mesh=finer,
        in_specs=in_specs,
        out_specs=(P(MP, ("dp", "space")),) * 4,
        check_vma=False,
    )
```

```python
import jax
import jax.numpy as jnp
from jax import lax
from jax.experimental import pallas as pl
from jax.experimental.pallas import tpu as pltpu
from jax.sharding import Mesh
from jax.sharding import PartitionSpec as P


MP = ("mp_0", "mp_1")
EPSILON = 1e-06
BF = jnp.bfloat16
F32 = jnp.float32
LANES = 128
GRANT = 12 * 1024 * 1024
NECK_ROWS = 16
SHARES = 2
PER_SHARE = 6


MEMBERS = 16
GATHER_ORDER = tuple((m + 10) % MEMBERS for m in range(MEMBERS))
SPREAD_ORDER = tuple(range(MEMBERS))
RETURN_ORDER = tuple((m + 10) % MEMBERS for m in range(MEMBERS))


def place(index, order):
    return order.index(index)


def exchanged(blocks, order):
    return lax.all_to_all(blocks, MP, 0, 0, tiled=True, axis_index_groups=[list(order)])


def by_source(blocks, order):
    places = [place(m, order) for m in range(MEMBERS)]
    return jnp.concatenate([blocks[k : k + 1] for k in places], axis=0)


def dot(a, b):
    return jnp.dot(a, b, preferred_element_type=F32)


def iota(shape, dim):
    return lax.broadcasted_iota(jnp.int32, shape, dim)


def one_hot(shape, source_of_column):
    rows = iota(shape, 0)
    columns = iota(shape, 1)
    return jnp.where(rows == source_of_column(columns), 1.0, 0.0).astype(BF)


def channel_norm(values, gain, shift):
    count = values.shape[0]
    center = jnp.sum(values, axis=0, keepdims=True) / count
    spread = jnp.sum(values * values, axis=0, keepdims=True) / count - center * center
    return (values - center) * lax.rsqrt(spread + EPSILON) * gain + shift


def weight_piece(halves, index):
    share, at = index // PER_SHARE, index % PER_SHARE
    return jnp.concatenate(
        [
            half[share][:, at * NECK_ROWS : (at + 1) * NECK_ROWS].reshape(-1, LANES)
            for half in halves
        ],
        axis=1,
    )


def spread_features(
    band_at, parity_at, x_from, conv_from, lat_from, bias_from, deconv_from, coarse_from,
    out, pair_out, half_out, x, conv, lat, bias, arrived,
):
    end = deconv_from.shape[0]
    ends = end + coarse_from.shape[0]
    copies = [
        pltpu.make_async_copy(source, target, arrived.at[k])
        for k, (source, target) in enumerate(
            (
                (x_from, x),
                (conv_from.at[0], conv),
                (lat_from, lat),
                (bias_from, bias),
                (deconv_from, pair_out.at[:end]),
                (coarse_from, pair_out.at[end:ends]),
            )
        )
    ]
    for copy in copies:
        copy.start()
    for copy in copies[:4]:
        copy.wait()
    members = out.shape[0]
    first = band_at[0] == 0
    even = parity_at[0] == 0
    columns = x.shape[1] // 2
    flats = []
    for h in range(2):
        part = x[:, h * columns : (h + 1) * columns].reshape(-1, x.shape[2])
        flat = part.astype(F32).T.astype(BF)
        flats.append(
            jnp.concatenate(
                [flat[:, k : k + LANES] for k in range(0, flat.shape[1], LANES)], axis=0
            )
        )
    half = lat.shape[1] // 2
    lateral = jnp.where(first, lat[:, :half], lat[:, half:])
    pieces = [jnp.where(first, conv[t, :, :LANES], conv[t, :, LANES:]) for t in range(9)]
    pieces += [lateral[:, :LANES], lateral[:, LANES:], lateral[:, LANES:]]
    weights = [jnp.where(even, pieces[k], pieces[PER_SHARE + k]) for k in range(PER_SHARE)]
    weights = jnp.concatenate(weights, axis=0)
    start = flats[0].shape[0]
    for m in range(members):
        at = place(m, GATHER_ORDER)
        out[at, :start] = flats[m % 2]
        out[at, start:] = weights
    rest = jnp.concatenate(
        [bias[...], jnp.zeros((1, LANES - bias.shape[1]), F32)], axis=1
    )
    parts = []
    for _ in range(3):
        parts.append(rest.astype(BF).astype(F32))
        rest = rest - parts[-1]
    parts = jnp.concatenate(parts + [jnp.zeros((NECK_ROWS - 3, LANES), F32)], axis=0)
    pair_out[ends:, :LANES] = parts.astype(BF)
    pair_out[ends:, LANES:] = jnp.zeros((NECK_ROWS, pair_out.shape[1] - LANES), BF)
    for copy in copies[4:]:
        copy.wait()
    half = half_out.shape[1]
    half_out[...] = jnp.where(first, pair_out[:, :half], pair_out[:, half:])


def join_halves(band_at, mine, theirs, out):
    first = band_at[0] == 0
    half = mine.shape[1]
    out[:, :half] = jnp.where(first, mine[...], theirs[...])
    out[:, half:] = jnp.where(first, theirs[...], mine[...])


def take_shares(gathered, share, share_low, share_high):
    half = gathered.shape[0] // 2
    split = gathered.shape[1] - share.shape[1]
    weights = by_source(gathered[:, split:], GATHER_ORDER)
    share[...] = weights
    share_low[...] = weights[:half]
    share_high[...] = weights[half:]


def raise_map(band_at, row_at, gathered, own, other, out, rows):
    members = gathered.shape[0]
    half_local = rows.shape[1]
    depth = own.shape[1]
    local = depth // members
    split = gathered.shape[1] - PER_SHARE * NECK_ROWS
    tiles = [
        by_source(gathered[:, k : k + local], GATHER_ORDER).reshape(depth, LANES)
        for k in range(0, split, local)
    ]
    x = jnp.concatenate(tiles, axis=1)
    columns = LANES // 4
    even = (row_at[0] & 1) == 0

    def of_pair(start, stop):
        mine, theirs = own[start:stop], other[start:stop]
        return jnp.where(even, mine, theirs), jnp.where(even, theirs, mine)

    end = 4 * half_local
    raised = [dot(weight, x) for weight in of_pair(0, end)]
    coarse_w = [of_pair(end + k * NECK_ROWS, end + (k + 1) * NECK_ROWS) for k in range(2)]
    diagonal = iota((half_local, half_local), 0) == iota((half_local, half_local), 1)
    biases = []
    for parts in of_pair(end + 2 * NECK_ROWS, own.shape[0]):
        parts = parts[:, :LANES].astype(F32)
        row = (parts[0:1] + parts[1:2] + parts[2:3])[:, :half_local]
        biases.append(jnp.sum(jnp.where(diagonal, row, 0.0), axis=1, keepdims=True))
    chunk = iota((half_local, LANES), 1) // columns
    for a in range(2):
        for t in range(len(tiles)):
            parts = [
                raised[k // 2][
                    (2 * a + k % 2) * half_local : (2 * a + k % 2 + 1) * half_local,
                    t * LANES : (t + 1) * LANES,
                ]
                + biases[k // 2]
                for k in range(4)
            ]
            for c in range(4):
                row = parts[c]
                for k in range(4):
                    if k != c:
                        moved = pltpu.roll(parts[k], (k - c) * columns % LANES, 1)
                        row = jnp.where(chunk == k, moved, row)
                rows[2 * (4 * t + c) + a] = row.astype(BF)
    middle = [dot(weight, x).astype(BF) for weight in coarse_w[0]]
    chunk = iota((depth, LANES), 1) // columns
    pairs = []
    for tile in tiles:
        tile = tile.astype(F32)
        pairs.append(jnp.maximum(tile, pltpu.roll(tile, LANES - columns, 1)))
    both = jnp.where(chunk % 2 == 0, pairs[0], pltpu.roll(pairs[1], columns, 1))
    pooled = jnp.maximum(both, pltpu.roll(both, LANES - 1, 1)).astype(BF)
    small = columns // 2
    coarse = 0.0
    for q, weight in enumerate(coarse_w[1]):
        values = dot(weight, pooled).astype(BF)

        def source(lane, q=q):
            row, at = (lane - q * 4 * small) // small, lane % small
            inside = (lane >= q * 4 * small) & (lane < (q + 1) * 4 * small)
            return jnp.where(inside, ((row % 2) * 2 + row // 2) * columns + 2 * at, -1)

        coarse = coarse + dot(values, one_hot((LANES, LANES), source))
    tail = [
        part[:, t * LANES : (t + 1) * LANES] for t in range(len(tiles)) for part in middle
    ] + [coarse.astype(BF)]
    tail = jnp.concatenate(tail, axis=0)
    first = band_at[0] == 0
    for m in range(members):
        row = jnp.where(first, m, members - 1 - m)
        at = place(m, SPREAD_ORDER)
        for k in range(3):
            out[at, k * half_local : (k + 1) * half_local] = rows[
                jnp.clip(row + k - 1, 0, members - 1)
            ]
        out[at, 3 * half_local :] = tail


def columns_of(gain, shift):
    blank = jnp.zeros((2, gain.shape[1]), F32)
    return jnp.concatenate([gain[...], blank, shift[...], blank], axis=0).T


def scaled(table, index):
    return table[:, index : index + 1], table[:, 8 + index : 9 + index]


def merge_shares(parity_at, own, low, high, out):
    parity = parity_at[0]
    middle = low.shape[0]
    out[parity] = own[...]
    out[1 - parity, :middle] = low[...]
    out[1 - parity, middle:] = high[...]


def lateral_weight(halves):
    pair = [weight_piece([half], 9 + k) for half in halves for k in range(2)]
    return jnp.concatenate(pair, axis=1)


def windows(center):
    lane = iota(center.shape, 1)
    columns = LANES // 4
    odd = lane // columns % 2 == 1
    at = lane % columns
    left = jnp.where(at == 0, pltpu.roll(center, 1, 1), pltpu.roll(center, LANES - columns + 1, 1))
    left = jnp.where(odd, pltpu.roll(center, columns, 1), left)
    left = jnp.where(lane == 0, 0.0, left)
    right = jnp.where(
        at == columns - 1, pltpu.roll(center, LANES - 1, 1), pltpu.roll(center, columns - 1, 1)
    )
    right = jnp.where(odd, right, pltpu.roll(center, LANES - columns, 1))
    right = jnp.where(lane == LANES - 1, 0.0, right)
    return [window.astype(BF) for window in (left, center, right)]


def paired(blocks):
    members, rows, _ = blocks.shape
    blocks = blocks.reshape(members // 2, 2, rows, LANES).astype(F32)
    sides = [blocks[:, h].reshape(-1, LANES) for h in range(2)]
    low = iota(sides[0].shape, 1) < LANES // 2
    near = jnp.where(low, sides[0], pltpu.roll(sides[1], LANES // 2, 1))
    far = jnp.where(low, pltpu.roll(sides[0], LANES // 2, 1), sides[1])
    both = [side.reshape(members // 2, 1, rows, LANES) for side in (near, far)]
    return jnp.concatenate(both, axis=1).reshape(members * rows, LANES)


def ordered_halves(first, mine, theirs):
    low = jnp.where(first, mine[...], theirs[...])
    high = jnp.where(first, theirs[...], mine[...])
    return low, high


def lateral_tile(source, k, start):
    base = start + k // 2 * 2 * NECK_ROWS
    blocks = by_source(source[:, base : base + 2 * NECK_ROWS], SPREAD_ORDER)
    blocks = blocks.reshape(-1, 2, 2 * NECK_ROWS, LANES).astype(F32)
    sides = [blocks[:, h].reshape(-1, LANES) for h in range(2)]
    columns = LANES // 4
    chunk = iota(sides[0].shape, 1) // columns
    tile = None
    for c in range(4):
        shift = (c - (2 * k + c // 2) % 4) * columns % LANES
        side = sides[c % 2]
        moved = pltpu.roll(side, shift, 1) if shift else side
        tile = moved if tile is None else jnp.where(chunk == c, moved, tile)
    return tile


def coarse_tile(source, start):
    base = start + 4 * NECK_ROWS
    rows = paired(by_source(source[:, base : base + NECK_ROWS], SPREAD_ORDER)).astype(BF)
    small = LANES // 8
    return dot(
        rows,
        one_hot(
            (LANES, LANES),
            lambda l: l % (2 * small) // small * (4 * small) + l // (2 * small) * small + l % small,
        ),
    )


def own_band(
    band_at, row_at, got, mine, theirs, conv, gain, shift,
    total_out, sixteen_out, thirty_out,
):
    members = got.shape[0]
    first = band_at[0] == 0
    row = jnp.where(first, row_at[0], members - 1 - row_at[0])
    half_local = (got.shape[1] - 5 * NECK_ROWS) // 3
    table = columns_of(gain, shift)
    halves = ordered_halves(first, mine, theirs)
    raised = jnp.concatenate(
        [
            paired(by_source(got[:, r * half_local : (r + 1) * half_local], SPREAD_ORDER)).astype(BF)
            for r in range(3)
        ],
        axis=1,
    )
    lat = dot(lateral_weight(halves), raised).astype(BF).astype(F32)
    normed = channel_norm(lat, *scaled(table, 0))
    total = None
    for r in range(3):
        center = normed[:, r * LANES : (r + 1) * LANES]
        if r == 0:
            center = jnp.where(row == 0, 0.0, center)
        if r == 2:
            center = jnp.where(row == members - 1, 0.0, center)
        for q, window in enumerate(windows(center)):
            part = dot(weight_piece(halves, 3 * r + q), window)
            total = part if total is None else total + part
    total_out[...] = total
    start = 3 * half_local
    middle = jnp.concatenate([lateral_tile(got, k, start) for k in range(4)], axis=1)
    normed = channel_norm(middle, *scaled(table, 2)).astype(BF)
    sixteen_out[...] = small_conv(normed, conv[1], LANES // 2)
    normed = channel_norm(coarse_tile(got, start), *scaled(table, 4)).astype(BF)
    thirty_out[...] = small_conv(normed, conv[2], LANES // 4)


def across(products, r, out_local, width):
    size = products.shape[1]
    column = iota((out_local, size), 1) % width
    pieces = [
        products[(3 * r + q) * out_local : (3 * r + q + 1) * out_local] for q in range(3)
    ]
    left = jnp.where(column == 0, 0.0, pltpu.roll(pieces[0], 1, 1))
    right = jnp.where(column == width - 1, 0.0, pltpu.roll(pieces[2], size - 1, 1))
    return left + pieces[1] + right


def small_conv(normed, weight, width):
    taps, out_local, depth = weight.shape
    products = dot(weight.reshape(taps * out_local, depth), normed)
    cells = normed.shape[1]
    lane = iota((out_local, cells), 1)
    above = pltpu.roll(across(products, 0, out_local, width), width, 1)
    below = pltpu.roll(across(products, 2, out_local, width), cells - width, 1)
    above = jnp.where(lane < width, 0.0, above)
    below = jnp.where(lane >= cells - width, 0.0, below)
    return above + across(products, 1, out_local, width) + below


def small_rim(total, halo, weight, width, first):
    taps, out_local, depth = weight.shape
    products = dot(weight.reshape(taps * out_local, depth), halo)
    cells = total.shape[1]
    lane = iota((out_local, LANES), 1)
    above = jnp.where(lane < width, across(products, 0, out_local, width), 0.0)
    below = jnp.where(lane < width, across(products, 2, out_local, width), 0.0)
    above = jnp.where(first, 0.0, above)
    below = jnp.where(first, pltpu.roll(below, LANES - width, 1), 0.0)
    if cells == LANES:
        return total + (above + below)
    return jnp.concatenate(
        [total[:, :LANES] + above, total[:, LANES : cells - LANES], total[:, cells - LANES :] + below],
        axis=1,
    )


def levels(
    band_at, row_at, got_other, total, total_sixteen, total_thirty, mine, theirs, conv, gain, shift,
    out, own_sixteen, own_thirty, own_table, table_at,
):
    members = got_other.shape[0]
    first = band_at[0] == 0
    half_local = (got_other.shape[1] - 5 * NECK_ROWS) // 3
    columns = LANES // 2
    table = columns_of(gain, shift)
    table_at[...] = table
    start = pl.multiple_of(row_at[0] * NECK_ROWS, NECK_ROWS)
    own_table[...] = table_at[pl.ds(start, NECK_ROWS), :]

    halves = ordered_halves(first, mine, theirs)
    raised = by_source(got_other[:, half_local : 2 * half_local], SPREAD_ORDER)
    raised = paired(raised).astype(BF)
    lat = dot(lateral_weight(halves), raised).astype(BF).astype(F32)
    center = channel_norm(lat, *scaled(table, 0))
    center = jnp.where(row_at[0] == members - 1, center, 0.0)
    convolved = total[...]
    for q, window in enumerate(windows(center)):
        tap = jnp.where(first, weight_piece(halves, 6 + q), weight_piece(halves, q))
        convolved = convolved + dot(tap, window)
    convolved = convolved.astype(BF).astype(F32)
    level = channel_norm(convolved, *scaled(table, 1)).astype(BF)
    mix = one_hot(
        (LANES, LANES), lambda l: l // columns * columns + (l % 2) * (columns // 2) + l % columns // 2
    )
    level = dot(level, mix).astype(BF).reshape(members, NECK_ROWS, LANES)
    for m in range(members):
        out[place(m, RETURN_ORDER), :NECK_ROWS] = level[m]

    start = 3 * half_local
    rim = lateral_tile(got_other, 3, start)
    rim = jnp.where(first, lateral_tile(got_other, 0, start), pltpu.roll(rim, columns, 1))
    normed = channel_norm(rim, *scaled(table, 2)).astype(BF)
    sixteen = small_rim(total_sixteen[...], normed, conv[1], columns, first).astype(BF)
    rim = coarse_tile(got_other, start)
    rim = jnp.where(first, rim, pltpu.roll(rim, columns // 2, 1))
    normed = channel_norm(rim, *scaled(table, 4)).astype(BF)
    thirty = small_rim(total_thirty[...], normed, conv[2], columns // 2, first).astype(BF)
    own_sixteen[...] = sixteen
    own_thirty[...] = thirty
    floats = jnp.concatenate([sixteen, thirty], axis=1).astype(F32)
    sums = jnp.sum(floats, axis=0, keepdims=True)
    squares = jnp.sum(floats * floats, axis=0, keepdims=True)
    pieces = floats.shape[1] // LANES
    stats = jnp.concatenate(
        [part[:, k * LANES : (k + 1) * LANES] for part in (sums, squares) for k in range(pieces)]
        ,
        axis=0,
    )
    parts = []
    for _ in range(3):
        parts.append(stats.astype(BF))
        stats = stats - parts[-1].astype(F32)
    parts.append(jnp.zeros((out.shape[1] - NECK_ROWS - 6 * pieces, LANES), BF))
    parts = jnp.concatenate([part.astype(F32) for part in parts], axis=0).astype(BF)
    for m in range(members):
        out[m, NECK_ROWS:] = parts


def finish(band_at, got, own_sixteen, own_thirty, table, eight, sixteen, thirty, sixty):
    members = got.shape[0]
    first = band_at[0] == 0
    neck = members * NECK_ROWS
    for r in range(members):
        source = jnp.where(
            first, place(r, RETURN_ORDER), place(members - 1 - r, RETURN_ORDER)
        )
        eight[:, r * LANES : (r + 1) * LANES] = got[source, :NECK_ROWS]
    stats = jnp.sum(got[:, NECK_ROWS:].astype(F32), axis=0)
    pieces = own_sixteen.shape[1] // LANES + 1
    stats = sum(stats[2 * pieces * k : 2 * pieces * (k + 1)] for k in range(3)) / neck

    def apply(values, k, index):
        gain, shift = scaled(table, index)
        center = stats[k : k + 1]
        spread = stats[pieces + k : pieces + k + 1] - center * center
        return ((values.astype(F32) - center) * lax.rsqrt(spread + EPSILON) * gain + shift).astype(BF)

    for k in range(pieces - 1):
        at = slice(k * LANES, (k + 1) * LANES)
        sixteen[:, at] = apply(own_sixteen[:, at], k, 3)
    last = apply(own_thirty[...], pieces - 1, 5)
    thirty[...] = last
    small = LANES // 4
    pick = one_hot(
        (LANES, sixty.shape[1]),
        lambda l: (l // (small // 2)) * (2 * small) + (l % (small // 2)) * 2,
    )
    sixty[...] = dot(last, pick).astype(BF)


def call(kernel, outs, where, *operands, scratch=(), space=pltpu.VMEM):
    spaces = space if isinstance(space, tuple) else (space,) * len(operands)
    specs = [pl.BlockSpec(memory_space=pltpu.SMEM) for _ in where] + [
        pl.BlockSpec(memory_space=space) for space in spaces
    ]
    return pl.pallas_call(
        kernel,
        in_specs=specs,
        out_specs=jax.tree.map(lambda _: pl.BlockSpec(memory_space=pltpu.VMEM), outs),
        out_shape=outs,
        scratch_shapes=scratch,
        compiler_params=pltpu.CompilerParams(vmem_limit_bytes=GRANT),
    )(*where, *map(pltpu.with_memory_space_constraint, operands, spaces))


def per_device(
    features,
    deconv_weight,
    deconv_bias,
    lateral_eight,
    lateral_coarse,
    output_conv,
    norm_gain,
    norm_shift,
):
    row_count, col_count, local = features.shape
    members = lax.axis_size(MP)
    pixels = row_count * col_count
    half_local = deconv_weight.shape[1]
    neck = norm_gain.shape[1]
    assert members == MEMBERS == 2 * row_count and 2 * col_count == LANES
    assert lateral_eight.shape[0] == NECK_ROWS and members * NECK_ROWS == neck
    shape = jax.ShapeDtypeStruct
    band, row, plane = (
        lax.axis_index(axis).astype(jnp.int32).reshape(1) for axis in ("space", MP, "dp")
    )
    planes = lax.axis_size("dp")
    assert planes % SHARES == 0
    parity = plane & 1
    conv = output_conv.transpose(0, 2, 1, 3)
    share_rows = PER_SHARE * NECK_ROWS

    def from_plane(value, step):
        return lax.ppermute(value, "dp", [((i + step) % planes, i) for i in range(planes)])

    def from_core(value):
        return lax.ppermute(value, "space", [(0, 1), (1, 0)])

    bias = deconv_bias.reshape(1, half_local)
    depth = deconv_weight.shape[2]
    kept = (features, conv, lateral_eight, bias)
    sent = (deconv_weight.reshape(-1, depth), lateral_coarse.reshape(-1, depth))
    pair_rows = 4 * half_local + 3 * NECK_ROWS
    blocks, pair, pair_half = call(
        spread_features,
        (
            shape((members, local * pixels // 2 // LANES + share_rows, LANES), BF),
            shape((pair_rows, depth), BF),
            shape((pair_rows, depth // 2), BF),
        ),
        (band, parity), *kept, *sent,
        space=pltpu.HBM,
        scratch=[
            *(pltpu.VMEM(x.shape[k == 1 :], x.dtype) for k, x in enumerate(kept)),
            pltpu.SemaphoreType.DMA((len(kept) + len(sent),)),
        ],
    )
    pair_half = lax.ppermute(pair_half, MP, [(m, m ^ 1) for m in range(members)])
    gathered = exchanged(blocks, GATHER_ORDER)
    pair_other = call(
        join_halves, shape((pair_rows, depth), BF), (band,), pair_half, from_core(pair_half)
    )
    share, share_low, share_high = call(
        take_shares,
        tuple(shape((rows, share_rows, LANES), BF) for rows in (members, members // 2, members // 2)),
        (), gathered,
    )
    blocks = call(
        raise_map,
        shape((members, 3 * half_local + 5 * NECK_ROWS, LANES), BF),
        (band, row), gathered, pair, pair_other,
        scratch=[pltpu.VMEM((members, half_local, LANES), BF)],
    )
    got = exchanged(blocks, SPREAD_ORDER)
    share_low = from_plane(share_low, -1)
    share_high = from_plane(share_high, 1)
    mine = call(
        merge_shares,
        shape((SHARES, members, share_rows, LANES), BF),
        (parity,), share, share_low, share_high,
    )
    theirs = from_core(mine)
    got_other = from_core(got)
    where = (band, row)
    weights = (mine, theirs)
    total, total_sixteen, total_thirty = call(
        own_band,
        (
            shape((neck, LANES), F32),
            shape((NECK_ROWS, pixels), F32),
            shape((NECK_ROWS, pixels // 4), F32),
        ),
        where, got, *weights, conv, norm_gain, norm_shift,
    )
    blocks, own_sixteen, own_thirty, table = call(
        levels,
        (
            shape((members, 3 * NECK_ROWS, LANES), BF),
            shape((NECK_ROWS, pixels), BF),
            shape((NECK_ROWS, pixels // 4), BF),
            shape((NECK_ROWS, 16), F32),
        ),
        where, got_other, total, total_sixteen, total_thirty, *weights, conv, norm_gain, norm_shift,
        scratch=[pltpu.VMEM((neck, 16), F32)],
    )
    got = exchanged(blocks, RETURN_ORDER)
    return call(
        finish,
        (
            shape((NECK_ROWS, 4 * pixels), BF),
            shape((NECK_ROWS, pixels), BF),
            shape((NECK_ROWS, pixels // 4), BF),
            shape((NECK_ROWS, pixels // 16), BF),
        ),
        (band,), got, own_sixteen, own_thirty, table,
    )


def solution(mesh):
    finer = Mesh(
        mesh.devices.reshape(mesh.shape["dp"], mesh.shape["space"], 4, 4),
        ("dp", "space", "mp_0", "mp_1"),
    )
    in_specs = (
        P(("dp", "space"), None, MP),
        P(None, MP, None),
        P(MP),
        P(MP, None),
        P(None, MP, None),
        P(None, MP, None, None),
        P(),
        P(),
    )
    return jax.shard_map(
        per_device,
        mesh=finer,
        in_specs=in_specs,
        out_specs=(P(MP, ("dp", "space")),) * 4,
        check_vma=False,
    )
```

```python
import jax
import jax.numpy as jnp
from jax import lax
from jax.experimental import pallas as pl
from jax.experimental.pallas import tpu as pltpu
from jax.sharding import Mesh
from jax.sharding import PartitionSpec as P


MP = ("mp_0", "mp_1")
EPSILON = 1e-06
BF = jnp.bfloat16
F32 = jnp.float32
LANES = 128
GRANT = 12 * 1024 * 1024
NECK_ROWS = 16
SHARES = 2
PER_SHARE = 6


MEMBERS = 16
GATHER_ORDER = tuple((m + 10) % MEMBERS for m in range(MEMBERS))
SPREAD_ORDER = tuple(range(MEMBERS))
RETURN_ORDER = tuple((m + 10) % MEMBERS for m in range(MEMBERS))


def place(index, order):
    return order.index(index)


def exchanged(blocks, order):
    return lax.all_to_all(blocks, MP, 0, 0, tiled=True, axis_index_groups=[list(order)])


def by_source(blocks, order):
    places = [place(m, order) for m in range(MEMBERS)]
    return jnp.concatenate([blocks[k : k + 1] for k in places], axis=0)


def dot(a, b):
    return jnp.dot(a, b, preferred_element_type=F32)


def iota(shape, dim):
    return lax.broadcasted_iota(jnp.int32, shape, dim)


def one_hot(shape, source_of_column):
    rows = iota(shape, 0)
    columns = iota(shape, 1)
    return jnp.where(rows == source_of_column(columns), 1.0, 0.0).astype(BF)


def channel_norm(values, gain, shift):
    count = values.shape[0]
    center = jnp.sum(values, axis=0, keepdims=True) / count
    spread = jnp.sum(values * values, axis=0, keepdims=True) / count - center * center
    return (values - center) * lax.rsqrt(spread + EPSILON) * gain + shift


def weight_piece(halves, index):
    share, at = index // PER_SHARE, index % PER_SHARE
    return jnp.concatenate(
        [
            half[share][:, at * NECK_ROWS : (at + 1) * NECK_ROWS].reshape(-1, LANES)
            for half in halves
        ],
        axis=1,
    )


def spread_features(
    band_at, parity_at, x_from, conv_from, lat_from, bias_from, deconv_from, coarse_from,
    out, pair_out, half_out, x, conv, lat, bias, arrived, blocks, left,
):
    end = deconv_from.shape[0]
    ends = end + coarse_from.shape[0]
    copies = [
        pltpu.make_async_copy(source, target, arrived.at[k])
        for k, (source, target) in enumerate(
            (
                (x_from, x),
                (conv_from.at[0], conv),
                (lat_from, lat),
                (bias_from, bias),
                (deconv_from, pair_out.at[:end]),
                (coarse_from, pair_out.at[end:ends]),
            )
        )
    ]
    for copy in copies:
        copy.start()
    for copy in copies[:4]:
        copy.wait()
    members = out.shape[0]
    first = band_at[0] == 0
    even = parity_at[0] == 0
    columns = x.shape[1] // 2
    flats = []
    for h in range(2):
        part = x[:, h * columns : (h + 1) * columns].reshape(-1, x.shape[2])
        flat = part.astype(F32).T.astype(BF)
        flats.append(
            jnp.concatenate(
                [flat[:, k : k + LANES] for k in range(0, flat.shape[1], LANES)], axis=0
            )
        )
    half = lat.shape[1] // 2
    lateral = jnp.where(first, lat[:, :half], lat[:, half:])
    pieces = [jnp.where(first, conv[t, :, :LANES], conv[t, :, LANES:]) for t in range(9)]
    pieces += [lateral[:, :LANES], lateral[:, LANES:], lateral[:, LANES:]]
    weights = [jnp.where(even, pieces[k], pieces[PER_SHARE + k]) for k in range(PER_SHARE)]
    weights = jnp.concatenate(weights, axis=0)
    start = flats[0].shape[0]
    for h in range(2):
        blocks[h, :start] = flats[h]
        blocks[h, start:] = weights
    leaving = []
    for m in range(members):
        target = out.at[place(m, GATHER_ORDER)]
        leaving.append(pltpu.make_async_copy(blocks.at[m % 2], target, left.at[m]))
        leaving[-1].start()
    rest = jnp.concatenate(
        [bias[...], jnp.zeros((1, LANES - bias.shape[1]), F32)], axis=1
    )
    parts = []
    for _ in range(3):
        parts.append(rest.astype(BF).astype(F32))
        rest = rest - parts[-1]
    parts = jnp.concatenate(parts + [jnp.zeros((NECK_ROWS - 3, LANES), F32)], axis=0)
    pair_out[ends:, :LANES] = parts.astype(BF)
    pair_out[ends:, LANES:] = jnp.zeros((NECK_ROWS, pair_out.shape[1] - LANES), BF)
    for copy in copies[4:]:
        copy.wait()
    half = half_out.shape[1]
    half_out[...] = jnp.where(first, pair_out[:, :half], pair_out[:, half:])
    for copy in leaving:
        copy.wait()


def join_halves(band_at, mine, theirs, out):
    first = band_at[0] == 0
    half = mine.shape[1]
    out[:, :half] = jnp.where(first, mine[...], theirs[...])
    out[:, half:] = jnp.where(first, theirs[...], mine[...])


def take_shares(gathered, share, share_low, share_high):
    half = gathered.shape[0] // 2
    split = gathered.shape[1] - share.shape[1]
    weights = by_source(gathered[:, split:], GATHER_ORDER)
    share[...] = weights
    share_low[...] = weights[:half]
    share_high[...] = weights[half:]


def raise_map(band_at, row_at, gathered, own, other, out, rows, blocks, left):
    members = gathered.shape[0]
    half_local = rows.shape[1]
    depth = own.shape[1]
    local = depth // members
    split = gathered.shape[1] - PER_SHARE * NECK_ROWS
    tiles = [
        by_source(gathered[:, k : k + local], GATHER_ORDER).reshape(depth, LANES)
        for k in range(0, split, local)
    ]
    x = jnp.concatenate(tiles, axis=1)
    columns = LANES // 4
    even = (row_at[0] & 1) == 0

    def of_pair(start, stop):
        mine, theirs = own[start:stop], other[start:stop]
        return jnp.where(even, mine, theirs), jnp.where(even, theirs, mine)

    end = 4 * half_local
    raised = [dot(weight, x) for weight in of_pair(0, end)]
    coarse_w = [of_pair(end + k * NECK_ROWS, end + (k + 1) * NECK_ROWS) for k in range(2)]
    diagonal = iota((half_local, half_local), 0) == iota((half_local, half_local), 1)
    biases = []
    for parts in of_pair(end + 2 * NECK_ROWS, own.shape[0]):
        parts = parts[:, :LANES].astype(F32)
        row = (parts[0:1] + parts[1:2] + parts[2:3])[:, :half_local]
        biases.append(jnp.sum(jnp.where(diagonal, row, 0.0), axis=1, keepdims=True))
    chunk = iota((half_local, LANES), 1) // columns
    for a in range(2):
        for t in range(len(tiles)):
            parts = [
                raised[k // 2][
                    (2 * a + k % 2) * half_local : (2 * a + k % 2 + 1) * half_local,
                    t * LANES : (t + 1) * LANES,
                ]
                + biases[k // 2]
                for k in range(4)
            ]
            for c in range(4):
                row = parts[c]
                for k in range(4):
                    if k != c:
                        moved = pltpu.roll(parts[k], (k - c) * columns % LANES, 1)
                        row = jnp.where(chunk == k, moved, row)
                rows[2 * (4 * t + c) + a] = row.astype(BF)
    middle = [dot(weight, x).astype(BF) for weight in coarse_w[0]]
    chunk = iota((depth, LANES), 1) // columns
    pairs = []
    for tile in tiles:
        tile = tile.astype(F32)
        pairs.append(jnp.maximum(tile, pltpu.roll(tile, LANES - columns, 1)))
    both = jnp.where(chunk % 2 == 0, pairs[0], pltpu.roll(pairs[1], columns, 1))
    pooled = jnp.maximum(both, pltpu.roll(both, LANES - 1, 1)).astype(BF)
    small = columns // 2
    coarse = 0.0
    for q, weight in enumerate(coarse_w[1]):
        values = dot(weight, pooled).astype(BF)

        def source(lane, q=q):
            row, at = (lane - q * 4 * small) // small, lane % small
            inside = (lane >= q * 4 * small) & (lane < (q + 1) * 4 * small)
            return jnp.where(inside, ((row % 2) * 2 + row // 2) * columns + 2 * at, -1)

        coarse = coarse + dot(values, one_hot((LANES, LANES), source))
    tail = [
        part[:, t * LANES : (t + 1) * LANES] for t in range(len(tiles)) for part in middle
    ] + [coarse.astype(BF)]
    tail = jnp.concatenate(tail, axis=0)
    first = band_at[0] == 0
    leaving = []
    for m in range(members):
        row = jnp.where(first, m, members - 1 - m)
        at = place(m, SPREAD_ORDER)
        for k in range(3):
            blocks[at, k * half_local : (k + 1) * half_local] = rows[
                jnp.clip(row + k - 1, 0, members - 1)
            ]
        blocks[at, 3 * half_local :] = tail
        leaving.append(pltpu.make_async_copy(blocks.at[at], out.at[at], left.at[at]))
        leaving[-1].start()
    for copy in leaving:
        copy.wait()


def columns_of(gain, shift):
    blank = jnp.zeros((2, gain.shape[1]), F32)
    return jnp.concatenate([gain[...], blank, shift[...], blank], axis=0).T


def scaled(table, index):
    return table[:, index : index + 1], table[:, 8 + index : 9 + index]


def merge_shares(parity_at, own, low, high, out):
    parity = parity_at[0]
    middle = low.shape[0]
    out[parity] = own[...]
    out[1 - parity, :middle] = low[...]
    out[1 - parity, middle:] = high[...]


def lateral_weight(halves):
    pair = [weight_piece([half], 9 + k) for half in halves for k in range(2)]
    return jnp.concatenate(pair, axis=1)


def windows(center):
    lane = iota(center.shape, 1)
    columns = LANES // 4
    odd = lane // columns % 2 == 1
    at = lane % columns
    left = jnp.where(at == 0, pltpu.roll(center, 1, 1), pltpu.roll(center, LANES - columns + 1, 1))
    left = jnp.where(odd, pltpu.roll(center, columns, 1), left)
    left = jnp.where(lane == 0, 0.0, left)
    right = jnp.where(
        at == columns - 1, pltpu.roll(center, LANES - 1, 1), pltpu.roll(center, columns - 1, 1)
    )
    right = jnp.where(odd, right, pltpu.roll(center, LANES - columns, 1))
    right = jnp.where(lane == LANES - 1, 0.0, right)
    return [window.astype(BF) for window in (left, center, right)]


def paired(blocks):
    members, rows, _ = blocks.shape
    blocks = blocks.reshape(members // 2, 2, rows, LANES).astype(F32)
    sides = [blocks[:, h].reshape(-1, LANES) for h in range(2)]
    low = iota(sides[0].shape, 1) < LANES // 2
    near = jnp.where(low, sides[0], pltpu.roll(sides[1], LANES // 2, 1))
    far = jnp.where(low, pltpu.roll(sides[0], LANES // 2, 1), sides[1])
    both = [side.reshape(members // 2, 1, rows, LANES) for side in (near, far)]
    return jnp.concatenate(both, axis=1).reshape(members * rows, LANES)


def ordered_halves(first, mine, theirs):
    low = jnp.where(first, mine[...], theirs[...])
    high = jnp.where(first, theirs[...], mine[...])
    return low, high


def lateral_tile(source, k, start):
    base = start + k // 2 * 2 * NECK_ROWS
    blocks = by_source(source[:, base : base + 2 * NECK_ROWS], SPREAD_ORDER)
    blocks = blocks.reshape(-1, 2, 2 * NECK_ROWS, LANES).astype(F32)
    sides = [blocks[:, h].reshape(-1, LANES) for h in range(2)]
    columns = LANES // 4
    chunk = iota(sides[0].shape, 1) // columns
    tile = None
    for c in range(4):
        shift = (c - (2 * k + c // 2) % 4) * columns % LANES
        side = sides[c % 2]
        moved = pltpu.roll(side, shift, 1) if shift else side
        tile = moved if tile is None else jnp.where(chunk == c, moved, tile)
    return tile


def coarse_tile(source, start):
    base = start + 4 * NECK_ROWS
    rows = paired(by_source(source[:, base : base + NECK_ROWS], SPREAD_ORDER)).astype(BF)
    small = LANES // 8
    return dot(
        rows,
        one_hot(
            (LANES, LANES),
            lambda l: l % (2 * small) // small * (4 * small) + l // (2 * small) * small + l % small,
        ),
    )


def own_band(
    band_at, row_at, got, mine, theirs, conv, gain, shift,
    total_out, sixteen_out, thirty_out,
):
    members = got.shape[0]
    first = band_at[0] == 0
    row = jnp.where(first, row_at[0], members - 1 - row_at[0])
    half_local = (got.shape[1] - 5 * NECK_ROWS) // 3
    table = columns_of(gain, shift)
    halves = ordered_halves(first, mine, theirs)
    raised = jnp.concatenate(
        [
            paired(by_source(got[:, r * half_local : (r + 1) * half_local], SPREAD_ORDER)).astype(BF)
            for r in range(3)
        ],
        axis=1,
    )
    lat = dot(lateral_weight(halves), raised).astype(BF).astype(F32)
    normed = channel_norm(lat, *scaled(table, 0))
    total = None
    for r in range(3):
        center = normed[:, r * LANES : (r + 1) * LANES]
        if r == 0:
            center = jnp.where(row == 0, 0.0, center)
        if r == 2:
            center = jnp.where(row == members - 1, 0.0, center)
        for q, window in enumerate(windows(center)):
            part = dot(weight_piece(halves, 3 * r + q), window)
            total = part if total is None else total + part
    total_out[...] = total
    start = 3 * half_local
    middle = jnp.concatenate([lateral_tile(got, k, start) for k in range(4)], axis=1)
    normed = channel_norm(middle, *scaled(table, 2)).astype(BF)
    sixteen_out[...] = small_conv(normed, conv[1], LANES // 2)
    normed = channel_norm(coarse_tile(got, start), *scaled(table, 4)).astype(BF)
    thirty_out[...] = small_conv(normed, conv[2], LANES // 4)


def across(products, r, out_local, width):
    size = products.shape[1]
    column = iota((out_local, size), 1) % width
    pieces = [
        products[(3 * r + q) * out_local : (3 * r + q + 1) * out_local] for q in range(3)
    ]
    left = jnp.where(column == 0, 0.0, pltpu.roll(pieces[0], 1, 1))
    right = jnp.where(column == width - 1, 0.0, pltpu.roll(pieces[2], size - 1, 1))
    return left + pieces[1] + right


def small_conv(normed, weight, width):
    taps, out_local, depth = weight.shape
    products = dot(weight.reshape(taps * out_local, depth), normed)
    cells = normed.shape[1]
    lane = iota((out_local, cells), 1)
    above = pltpu.roll(across(products, 0, out_local, width), width, 1)
    below = pltpu.roll(across(products, 2, out_local, width), cells - width, 1)
    above = jnp.where(lane < width, 0.0, above)
    below = jnp.where(lane >= cells - width, 0.0, below)
    return above + across(products, 1, out_local, width) + below


def small_rim(total, halo, weight, width, first):
    taps, out_local, depth = weight.shape
    products = dot(weight.reshape(taps * out_local, depth), halo)
    cells = total.shape[1]
    lane = iota((out_local, LANES), 1)
    above = jnp.where(lane < width, across(products, 0, out_local, width), 0.0)
    below = jnp.where(lane < width, across(products, 2, out_local, width), 0.0)
    above = jnp.where(first, 0.0, above)
    below = jnp.where(first, pltpu.roll(below, LANES - width, 1), 0.0)
    if cells == LANES:
        return total + (above + below)
    return jnp.concatenate(
        [total[:, :LANES] + above, total[:, LANES : cells - LANES], total[:, cells - LANES :] + below],
        axis=1,
    )


def levels(
    band_at, row_at, got_other, total, total_sixteen, total_thirty, mine, theirs, conv, gain, shift,
    out, own_sixteen, own_thirty, own_table, table_at,
):
    members = got_other.shape[0]
    first = band_at[0] == 0
    half_local = (got_other.shape[1] - 5 * NECK_ROWS) // 3
    columns = LANES // 2
    table = columns_of(gain, shift)
    table_at[...] = table
    start = pl.multiple_of(row_at[0] * NECK_ROWS, NECK_ROWS)
    own_table[...] = table_at[pl.ds(start, NECK_ROWS), :]

    halves = ordered_halves(first, mine, theirs)
    raised = by_source(got_other[:, half_local : 2 * half_local], SPREAD_ORDER)
    raised = paired(raised).astype(BF)
    lat = dot(lateral_weight(halves), raised).astype(BF).astype(F32)
    center = channel_norm(lat, *scaled(table, 0))
    center = jnp.where(row_at[0] == members - 1, center, 0.0)
    convolved = total[...]
    for q, window in enumerate(windows(center)):
        tap = jnp.where(first, weight_piece(halves, 6 + q), weight_piece(halves, q))
        convolved = convolved + dot(tap, window)
    convolved = convolved.astype(BF).astype(F32)
    level = channel_norm(convolved, *scaled(table, 1)).astype(BF)
    mix = one_hot(
        (LANES, LANES), lambda l: l // columns * columns + (l % 2) * (columns // 2) + l % columns // 2
    )
    level = dot(level, mix).astype(BF).reshape(members, NECK_ROWS, LANES)
    for m in range(members):
        out[place(m, RETURN_ORDER), :NECK_ROWS] = level[m]

    start = 3 * half_local
    rim = lateral_tile(got_other, 3, start)
    rim = jnp.where(first, lateral_tile(got_other, 0, start), pltpu.roll(rim, columns, 1))
    normed = channel_norm(rim, *scaled(table, 2)).astype(BF)
    sixteen = small_rim(total_sixteen[...], normed, conv[1], columns, first).astype(BF)
    rim = coarse_tile(got_other, start)
    rim = jnp.where(first, rim, pltpu.roll(rim, columns // 2, 1))
    normed = channel_norm(rim, *scaled(table, 4)).astype(BF)
    thirty = small_rim(total_thirty[...], normed, conv[2], columns // 2, first).astype(BF)
    own_sixteen[...] = sixteen
    own_thirty[...] = thirty
    floats = jnp.concatenate([sixteen, thirty], axis=1).astype(F32)
    sums = jnp.sum(floats, axis=0, keepdims=True)
    squares = jnp.sum(floats * floats, axis=0, keepdims=True)
    pieces = floats.shape[1] // LANES
    stats = jnp.concatenate(
        [part[:, k * LANES : (k + 1) * LANES] for part in (sums, squares) for k in range(pieces)]
        ,
        axis=0,
    )
    parts = []
    for _ in range(3):
        parts.append(stats.astype(BF))
        stats = stats - parts[-1].astype(F32)
    parts.append(jnp.zeros((out.shape[1] - NECK_ROWS - 6 * pieces, LANES), BF))
    parts = jnp.concatenate([part.astype(F32) for part in parts], axis=0).astype(BF)
    for m in range(members):
        out[m, NECK_ROWS:] = parts


def finish(band_at, got, own_sixteen, own_thirty, table, eight, sixteen, thirty, sixty):
    members = got.shape[0]
    first = band_at[0] == 0
    neck = members * NECK_ROWS
    for r in range(members):
        source = jnp.where(
            first, place(r, RETURN_ORDER), place(members - 1 - r, RETURN_ORDER)
        )
        eight[:, r * LANES : (r + 1) * LANES] = got[source, :NECK_ROWS]
    stats = jnp.sum(got[:, NECK_ROWS:].astype(F32), axis=0)
    pieces = own_sixteen.shape[1] // LANES + 1
    stats = sum(stats[2 * pieces * k : 2 * pieces * (k + 1)] for k in range(3)) / neck

    def apply(values, k, index):
        gain, shift = scaled(table, index)
        center = stats[k : k + 1]
        spread = stats[pieces + k : pieces + k + 1] - center * center
        return ((values.astype(F32) - center) * lax.rsqrt(spread + EPSILON) * gain + shift).astype(BF)

    for k in range(pieces - 1):
        at = slice(k * LANES, (k + 1) * LANES)
        sixteen[:, at] = apply(own_sixteen[:, at], k, 3)
    last = apply(own_thirty[...], pieces - 1, 5)
    thirty[...] = last
    small = LANES // 4
    pick = one_hot(
        (LANES, sixty.shape[1]),
        lambda l: (l // (small // 2)) * (2 * small) + (l % (small // 2)) * 2,
    )
    sixty[...] = dot(last, pick).astype(BF)


def call(kernel, outs, where, *operands, scratch=(), space=pltpu.VMEM, direct=False):
    spaces = space if isinstance(space, tuple) else (space,) * len(operands)
    specs = [pl.BlockSpec(memory_space=pltpu.SMEM) for _ in where] + [
        pl.BlockSpec(memory_space=space) for space in spaces
    ]
    return pl.pallas_call(
        kernel,
        in_specs=specs,
        out_specs=jax.tree.unflatten(
            jax.tree.structure(outs),
            [
                pl.BlockSpec(memory_space=pltpu.HBM if direct and k == 0 else pltpu.VMEM)
                for k in range(len(jax.tree.leaves(outs)))
            ],
        ),
        out_shape=outs,
        scratch_shapes=scratch,
        compiler_params=pltpu.CompilerParams(vmem_limit_bytes=GRANT),
    )(*where, *map(pltpu.with_memory_space_constraint, operands, spaces))


def per_device(
    features,
    deconv_weight,
    deconv_bias,
    lateral_eight,
    lateral_coarse,
    output_conv,
    norm_gain,
    norm_shift,
):
    row_count, col_count, local = features.shape
    members = lax.axis_size(MP)
    pixels = row_count * col_count
    half_local = deconv_weight.shape[1]
    neck = norm_gain.shape[1]
    assert members == MEMBERS == 2 * row_count and 2 * col_count == LANES
    assert lateral_eight.shape[0] == NECK_ROWS and members * NECK_ROWS == neck
    shape = jax.ShapeDtypeStruct
    band, row, plane = (
        lax.axis_index(axis).astype(jnp.int32).reshape(1) for axis in ("space", MP, "dp")
    )
    planes = lax.axis_size("dp")
    assert planes % SHARES == 0
    parity = plane & 1
    conv = output_conv.transpose(0, 2, 1, 3)
    share_rows = PER_SHARE * NECK_ROWS

    def from_plane(value, step):
        return lax.ppermute(value, "dp", [((i + step) % planes, i) for i in range(planes)])

    def from_core(value):
        return lax.ppermute(value, "space", [(0, 1), (1, 0)])

    bias = deconv_bias.reshape(1, half_local)
    depth = deconv_weight.shape[2]
    kept = (features, conv, lateral_eight, bias)
    sent = (deconv_weight.reshape(-1, depth), lateral_coarse.reshape(-1, depth))
    pair_rows = 4 * half_local + 3 * NECK_ROWS
    blocks, pair, pair_half = call(
        spread_features,
        (
            shape((members, local * pixels // 2 // LANES + share_rows, LANES), BF),
            shape((pair_rows, depth), BF),
            shape((pair_rows, depth // 2), BF),
        ),
        (band, parity), *kept, *sent,
        space=pltpu.HBM,
        direct=True,
        scratch=[
            *(pltpu.VMEM(x.shape[k == 1 :], x.dtype) for k, x in enumerate(kept)),
            pltpu.SemaphoreType.DMA((len(kept) + len(sent),)),
            pltpu.VMEM((2, local * pixels // 2 // LANES + share_rows, LANES), BF),
            pltpu.SemaphoreType.DMA((members,)),
        ],
    )
    pair_half = lax.ppermute(pair_half, MP, [(m, m ^ 1) for m in range(members)])
    gathered = exchanged(blocks, GATHER_ORDER)
    pair_other = call(
        join_halves, shape((pair_rows, depth), BF), (band,), pair_half, from_core(pair_half)
    )
    share, share_low, share_high = call(
        take_shares,
        tuple(shape((rows, share_rows, LANES), BF) for rows in (members, members // 2, members // 2)),
        (), gathered,
    )
    blocks = call(
        raise_map,
        shape((members, 3 * half_local + 5 * NECK_ROWS, LANES), BF),
        (band, row), gathered, pair, pair_other,
        scratch=[
            pltpu.VMEM((members, half_local, LANES), BF),
            pltpu.VMEM((members, 3 * half_local + 5 * NECK_ROWS, LANES), BF),
            pltpu.SemaphoreType.DMA((members,)),
        ],
        direct=True,
    )
    got = exchanged(blocks, SPREAD_ORDER)
    share_low = from_plane(share_low, -1)
    share_high = from_plane(share_high, 1)
    mine = call(
        merge_shares,
        shape((SHARES, members, share_rows, LANES), BF),
        (parity,), share, share_low, share_high,
    )
    theirs = from_core(mine)
    got_other = from_core(got)
    where = (band, row)
    weights = (mine, theirs)
    total, total_sixteen, total_thirty = call(
        own_band,
        (
            shape((neck, LANES), F32),
            shape((NECK_ROWS, pixels), F32),
            shape((NECK_ROWS, pixels // 4), F32),
        ),
        where, got, *weights, conv, norm_gain, norm_shift,
    )
    blocks, own_sixteen, own_thirty, table = call(
        levels,
        (
            shape((members, 3 * NECK_ROWS, LANES), BF),
            shape((NECK_ROWS, pixels), BF),
            shape((NECK_ROWS, pixels // 4), BF),
            shape((NECK_ROWS, 16), F32),
        ),
        where, got_other, total, total_sixteen, total_thirty, *weights, conv, norm_gain, norm_shift,
        scratch=[pltpu.VMEM((neck, 16), F32)],
    )
    got = exchanged(blocks, RETURN_ORDER)
    return call(
        finish,
        (
            shape((NECK_ROWS, 4 * pixels), BF),
            shape((NECK_ROWS, pixels), BF),
            shape((NECK_ROWS, pixels // 4), BF),
            shape((NECK_ROWS, pixels // 16), BF),
        ),
        (band,), got, own_sixteen, own_thirty, table,
    )


def solution(mesh):
    finer = Mesh(
        mesh.devices.reshape(mesh.shape["dp"], mesh.shape["space"], 4, 4),
        ("dp", "space", "mp_0", "mp_1"),
    )
    in_specs = (
        P(("dp", "space"), None, MP),
        P(None, MP, None),
        P(MP),
        P(MP, None),
        P(None, MP, None),
        P(None, MP, None, None),
        P(),
        P(),
    )
    return jax.shard_map(
        per_device,
        mesh=finer,
        in_specs=in_specs,
        out_specs=(P(MP, ("dp", "space")),) * 4,
        check_vma=False,
    )
```

```python
import jax
import jax.numpy as jnp
from jax import lax
from jax.experimental import pallas as pl
from jax.experimental.pallas import tpu as pltpu
from jax.sharding import Mesh
from jax.sharding import PartitionSpec as P


MP = ("mp_0", "mp_1")
EPSILON = 1e-06
BF = jnp.bfloat16
F32 = jnp.float32
LANES = 128
GRANT = 12 * 1024 * 1024
NECK_ROWS = 16
SHARES = 2
PER_SHARE = 6


MEMBERS = 16
GATHER_ORDER = tuple((m + 10) % MEMBERS for m in range(MEMBERS))
SPREAD_ORDER = tuple(range(MEMBERS))
RETURN_ORDER = tuple((m + 10) % MEMBERS for m in range(MEMBERS))


def place(index, order):
    return order.index(index)


def exchanged(blocks, order):
    return lax.all_to_all(blocks, MP, 0, 0, tiled=True, axis_index_groups=[list(order)])


def by_source(blocks, order):
    places = [place(m, order) for m in range(MEMBERS)]
    return jnp.concatenate([blocks[k : k + 1] for k in places], axis=0)


def dot(a, b):
    return jnp.dot(a, b, preferred_element_type=F32)


def iota(shape, dim):
    return lax.broadcasted_iota(jnp.int32, shape, dim)


def one_hot(shape, source_of_column):
    rows = iota(shape, 0)
    columns = iota(shape, 1)
    return jnp.where(rows == source_of_column(columns), 1.0, 0.0).astype(BF)


def channel_norm(values, gain, shift):
    count = values.shape[0]
    center = jnp.sum(values, axis=0, keepdims=True) / count
    spread = jnp.sum(values * values, axis=0, keepdims=True) / count - center * center
    return (values - center) * lax.rsqrt(spread + EPSILON) * gain + shift


def weight_piece(halves, index):
    share, at = index // PER_SHARE, index % PER_SHARE
    return jnp.concatenate(
        [
            half[share][:, at * NECK_ROWS : (at + 1) * NECK_ROWS].reshape(-1, LANES)
            for half in halves
        ],
        axis=1,
    )


def spread_features(
    band_at, parity_at, x_from, conv_from, lat_from, bias_from, deconv_from, coarse_from,
    out, pair_out, half_out, x, conv, lat, bias, arrived,
):
    end = deconv_from.shape[0]
    ends = end + coarse_from.shape[0]
    copies = [
        pltpu.make_async_copy(source, target, arrived.at[k])
        for k, (source, target) in enumerate(
            (
                (x_from, x),
                (conv_from.at[0], conv),
                (lat_from, lat),
                (bias_from, bias),
                (deconv_from, pair_out.at[:end]),
                (coarse_from, pair_out.at[end:ends]),
            )
        )
    ]
    for copy in copies:
        copy.start()
    for copy in copies[:4]:
        copy.wait()
    members = out.shape[0]
    first = band_at[0] == 0
    even = parity_at[0] == 0
    columns = x.shape[1] // 2
    flats = []
    for h in range(2):
        part = x[:, h * columns : (h + 1) * columns].reshape(-1, x.shape[2])
        flat = part.astype(F32).T.astype(BF)
        flats.append(
            jnp.concatenate(
                [flat[:, k : k + LANES] for k in range(0, flat.shape[1], LANES)], axis=0
            )
        )
    half = lat.shape[1] // 2
    lateral = jnp.where(first, lat[:, :half], lat[:, half:])
    pieces = [jnp.where(first, conv[t, :, :LANES], conv[t, :, LANES:]) for t in range(9)]
    pieces += [lateral[:, :LANES], lateral[:, LANES:], lateral[:, LANES:]]
    weights = [jnp.where(even, pieces[k], pieces[PER_SHARE + k]) for k in range(PER_SHARE)]
    weights = jnp.concatenate(weights, axis=0)
    start = flats[0].shape[0]
    for m in range(members):
        at = place(m, GATHER_ORDER)
        out[at, :start] = flats[m % 2]
        out[at, start:] = weights
    rest = jnp.concatenate(
        [bias[...], jnp.zeros((1, LANES - bias.shape[1]), F32)], axis=1
    )
    parts = []
    for _ in range(3):
        parts.append(rest.astype(BF).astype(F32))
        rest = rest - parts[-1]
    parts = jnp.concatenate(parts + [jnp.zeros((NECK_ROWS - 3, LANES), F32)], axis=0)
    pair_out[ends:, :LANES] = parts.astype(BF)
    pair_out[ends:, LANES:] = jnp.zeros((NECK_ROWS, pair_out.shape[1] - LANES), BF)
    for copy in copies[4:]:
        copy.wait()
    half = half_out.shape[1]
    half_out[...] = jnp.where(first, pair_out[:, :half], pair_out[:, half:])


def join_halves(band_at, mine, theirs, out):
    first = band_at[0] == 0
    half = mine.shape[1]
    out[:, :half] = jnp.where(first, mine[...], theirs[...])
    out[:, half:] = jnp.where(first, theirs[...], mine[...])


def take_shares(gathered, share, share_low, share_high):
    half = gathered.shape[0] // 2
    split = gathered.shape[1] - share.shape[1]
    weights = by_source(gathered[:, split:], GATHER_ORDER)
    share[...] = weights
    share_low[...] = weights[:half]
    share_high[...] = weights[half:]


def raise_map(band_at, row_at, gathered, own, other, out, rows):
    members = gathered.shape[0]
    half_local = rows.shape[1]
    depth = own.shape[1]
    local = depth // members
    split = gathered.shape[1] - PER_SHARE * NECK_ROWS
    tiles = [
        by_source(gathered[:, k : k + local], GATHER_ORDER).reshape(depth, LANES)
        for k in range(0, split, local)
    ]
    x = jnp.concatenate(tiles, axis=1)
    columns = LANES // 4
    even = (row_at[0] & 1) == 0

    def of_pair(start, stop):
        mine, theirs = own[start:stop], other[start:stop]
        return jnp.where(even, mine, theirs), jnp.where(even, theirs, mine)

    end = 4 * half_local
    raised = [dot(weight, x) for weight in of_pair(0, end)]
    coarse_w = [of_pair(end + k * NECK_ROWS, end + (k + 1) * NECK_ROWS) for k in range(2)]
    diagonal = iota((half_local, half_local), 0) == iota((half_local, half_local), 1)
    biases = []
    for parts in of_pair(end + 2 * NECK_ROWS, own.shape[0]):
        parts = parts[:, :LANES].astype(F32)
        row = (parts[0:1] + parts[1:2] + parts[2:3])[:, :half_local]
        biases.append(jnp.sum(jnp.where(diagonal, row, 0.0), axis=1, keepdims=True))
    chunk = iota((half_local, LANES), 1) // columns
    for a in range(2):
        for t in range(len(tiles)):
            parts = [
                raised[k // 2][
                    (2 * a + k % 2) * half_local : (2 * a + k % 2 + 1) * half_local,
                    t * LANES : (t + 1) * LANES,
                ]
                + biases[k // 2]
                for k in range(4)
            ]
            for c in range(4):
                row = parts[c]
                for k in range(4):
                    if k != c:
                        moved = pltpu.roll(parts[k], (k - c) * columns % LANES, 1)
                        row = jnp.where(chunk == k, moved, row)
                rows[2 * (4 * t + c) + a] = row.astype(BF)
    middle = [dot(weight, x).astype(BF) for weight in coarse_w[0]]
    chunk = iota((depth, LANES), 1) // columns
    pairs = []
    for tile in tiles:
        tile = tile.astype(F32)
        pairs.append(jnp.maximum(tile, pltpu.roll(tile, LANES - columns, 1)))
    both = jnp.where(chunk % 2 == 0, pairs[0], pltpu.roll(pairs[1], columns, 1))
    pooled = jnp.maximum(both, pltpu.roll(both, LANES - 1, 1)).astype(BF)
    small = columns // 2
    coarse = 0.0
    for q, weight in enumerate(coarse_w[1]):
        values = dot(weight, pooled).astype(BF)

        def source(lane, q=q):
            row, at = (lane - q * 4 * small) // small, lane % small
            inside = (lane >= q * 4 * small) & (lane < (q + 1) * 4 * small)
            return jnp.where(inside, ((row % 2) * 2 + row // 2) * columns + 2 * at, -1)

        coarse = coarse + dot(values, one_hot((LANES, LANES), source))
    tail = [
        part[:, t * LANES : (t + 1) * LANES] for t in range(len(tiles)) for part in middle
    ] + [coarse.astype(BF)]
    tail = jnp.concatenate(tail, axis=0)
    first = band_at[0] == 0
    for m in range(members):
        row = jnp.where(first, m, members - 1 - m)
        at = place(m, SPREAD_ORDER)
        for k in range(3):
            out[at, k * half_local : (k + 1) * half_local] = rows[
                jnp.clip(row + k - 1, 0, members - 1)
            ]
        out[at, 3 * half_local :] = tail


def columns_of(gain, shift):
    blank = jnp.zeros((2, gain.shape[1]), F32)
    return jnp.concatenate([gain[...], blank, shift[...], blank], axis=0).T


def scaled(table, index):
    return table[:, index : index + 1], table[:, 8 + index : 9 + index]


def merge_shares(parity_at, own, low, high, out):
    parity = parity_at[0]
    middle = low.shape[0]
    out[parity] = own[...]
    out[1 - parity, :middle] = low[...]
    out[1 - parity, middle:] = high[...]


def lateral_weight(halves):
    pair = [weight_piece([half], 9 + k) for half in halves for k in range(2)]
    return jnp.concatenate(pair, axis=1)


def windows(center):
    lane = iota(center.shape, 1)
    columns = LANES // 4
    odd = lane // columns % 2 == 1
    at = lane % columns
    left = jnp.where(at == 0, pltpu.roll(center, 1, 1), pltpu.roll(center, LANES - columns + 1, 1))
    left = jnp.where(odd, pltpu.roll(center, columns, 1), left)
    left = jnp.where(lane == 0, 0.0, left)
    right = jnp.where(
        at == columns - 1, pltpu.roll(center, LANES - 1, 1), pltpu.roll(center, columns - 1, 1)
    )
    right = jnp.where(odd, right, pltpu.roll(center, LANES - columns, 1))
    right = jnp.where(lane == LANES - 1, 0.0, right)
    return [window.astype(BF) for window in (left, center, right)]


def paired(blocks):
    members, rows, _ = blocks.shape
    blocks = blocks.reshape(members // 2, 2, rows, LANES)
    sides = [blocks[:, h].reshape(-1, LANES) for h in range(2)]
    middle = LANES // 2
    near = jnp.concatenate([side[:, :middle] for side in sides], axis=1)
    far = jnp.concatenate([side[:, middle:] for side in sides], axis=1)
    both = [side.reshape(members // 2, 1, rows, LANES) for side in (near, far)]
    return jnp.concatenate(both, axis=1).reshape(members * rows, LANES)


def ordered_halves(first, mine, theirs):
    low = jnp.where(first, mine[...], theirs[...])
    high = jnp.where(first, theirs[...], mine[...])
    return low, high


def lateral_tile(source, k, start):
    base = start + k // 2 * 2 * NECK_ROWS
    blocks = by_source(source[:, base : base + 2 * NECK_ROWS], SPREAD_ORDER)
    blocks = blocks.reshape(-1, 2, 2 * NECK_ROWS, LANES).astype(F32)
    sides = [blocks[:, h].reshape(-1, LANES) for h in range(2)]
    columns = LANES // 4
    chunk = iota(sides[0].shape, 1) // columns
    tile = None
    for c in range(4):
        shift = (c - (2 * k + c // 2) % 4) * columns % LANES
        side = sides[c % 2]
        moved = pltpu.roll(side, shift, 1) if shift else side
        tile = moved if tile is None else jnp.where(chunk == c, moved, tile)
    return tile


def coarse_tile(source, start):
    base = start + 4 * NECK_ROWS
    rows = paired(by_source(source[:, base : base + NECK_ROWS], SPREAD_ORDER)).astype(BF)
    small = LANES // 8
    return dot(
        rows,
        one_hot(
            (LANES, LANES),
            lambda l: l % (2 * small) // small * (4 * small) + l // (2 * small) * small + l % small,
        ),
    )


def own_band(
    band_at, row_at, got, mine, theirs, conv, gain, shift,
    total_out, sixteen_out, thirty_out,
):
    members = got.shape[0]
    first = band_at[0] == 0
    row = jnp.where(first, row_at[0], members - 1 - row_at[0])
    half_local = (got.shape[1] - 5 * NECK_ROWS) // 3
    table = columns_of(gain, shift)
    halves = ordered_halves(first, mine, theirs)
    raised = jnp.concatenate(
        [
            paired(by_source(got[:, r * half_local : (r + 1) * half_local], SPREAD_ORDER)).astype(BF)
            for r in range(3)
        ],
        axis=1,
    )
    lat = dot(lateral_weight(halves), raised).astype(BF).astype(F32)
    normed = channel_norm(lat, *scaled(table, 0))
    total = None
    for r in range(3):
        center = normed[:, r * LANES : (r + 1) * LANES]
        if r == 0:
            center = jnp.where(row == 0, 0.0, center)
        if r == 2:
            center = jnp.where(row == members - 1, 0.0, center)
        for q, window in enumerate(windows(center)):
            part = dot(weight_piece(halves, 3 * r + q), window)
            total = part if total is None else total + part
    total_out[...] = total
    start = 3 * half_local
    middle = jnp.concatenate([lateral_tile(got, k, start) for k in range(4)], axis=1)
    normed = channel_norm(middle, *scaled(table, 2)).astype(BF)
    sixteen_out[...] = small_conv(normed, conv[1], LANES // 2)
    normed = channel_norm(coarse_tile(got, start), *scaled(table, 4)).astype(BF)
    thirty_out[...] = small_conv(normed, conv[2], LANES // 4)


def across(products, r, out_local, width):
    size = products.shape[1]
    column = iota((out_local, size), 1) % width
    pieces = [
        products[(3 * r + q) * out_local : (3 * r + q + 1) * out_local] for q in range(3)
    ]
    left = jnp.where(column == 0, 0.0, pltpu.roll(pieces[0], 1, 1))
    right = jnp.where(column == width - 1, 0.0, pltpu.roll(pieces[2], size - 1, 1))
    return left + pieces[1] + right


def small_conv(normed, weight, width):
    taps, out_local, depth = weight.shape
    products = dot(weight.reshape(taps * out_local, depth), normed)
    cells = normed.shape[1]
    lane = iota((out_local, cells), 1)
    above = pltpu.roll(across(products, 0, out_local, width), width, 1)
    below = pltpu.roll(across(products, 2, out_local, width), cells - width, 1)
    above = jnp.where(lane < width, 0.0, above)
    below = jnp.where(lane >= cells - width, 0.0, below)
    return above + across(products, 1, out_local, width) + below


def small_rim(total, halo, weight, width, first):
    taps, out_local, depth = weight.shape
    products = dot(weight.reshape(taps * out_local, depth), halo)
    cells = total.shape[1]
    lane = iota((out_local, LANES), 1)
    above = jnp.where(lane < width, across(products, 0, out_local, width), 0.0)
    below = jnp.where(lane < width, across(products, 2, out_local, width), 0.0)
    above = jnp.where(first, 0.0, above)
    below = jnp.where(first, pltpu.roll(below, LANES - width, 1), 0.0)
    if cells == LANES:
        return total + (above + below)
    return jnp.concatenate(
        [total[:, :LANES] + above, total[:, LANES : cells - LANES], total[:, cells - LANES :] + below],
        axis=1,
    )


def levels(
    band_at, row_at, got_other, total, total_sixteen, total_thirty, mine, theirs, conv, gain, shift,
    out, own_sixteen, own_thirty, own_table, table_at,
):
    members = got_other.shape[0]
    first = band_at[0] == 0
    half_local = (got_other.shape[1] - 5 * NECK_ROWS) // 3
    columns = LANES // 2
    table = columns_of(gain, shift)
    table_at[...] = table
    start = pl.multiple_of(row_at[0] * NECK_ROWS, NECK_ROWS)
    own_table[...] = table_at[pl.ds(start, NECK_ROWS), :]

    halves = ordered_halves(first, mine, theirs)
    raised = by_source(got_other[:, half_local : 2 * half_local], SPREAD_ORDER)
    raised = paired(raised).astype(BF)
    lat = dot(lateral_weight(halves), raised).astype(BF).astype(F32)
    center = channel_norm(lat, *scaled(table, 0))
    center = jnp.where(row_at[0] == members - 1, center, 0.0)
    convolved = total[...]
    for q, window in enumerate(windows(center)):
        tap = jnp.where(first, weight_piece(halves, 6 + q), weight_piece(halves, q))
        convolved = convolved + dot(tap, window)
    convolved = convolved.astype(BF).astype(F32)
    level = channel_norm(convolved, *scaled(table, 1)).astype(BF)
    mix = one_hot(
        (LANES, LANES), lambda l: l // columns * columns + (l % 2) * (columns // 2) + l % columns // 2
    )
    level = dot(level, mix).astype(BF).reshape(members, NECK_ROWS, LANES)
    for m in range(members):
        out[place(m, RETURN_ORDER), :NECK_ROWS] = level[m]

    start = 3 * half_local
    rim = lateral_tile(got_other, 3, start)
    rim = jnp.where(first, lateral_tile(got_other, 0, start), pltpu.roll(rim, columns, 1))
    normed = channel_norm(rim, *scaled(table, 2)).astype(BF)
    sixteen = small_rim(total_sixteen[...], normed, conv[1], columns, first).astype(BF)
    rim = coarse_tile(got_other, start)
    rim = jnp.where(first, rim, pltpu.roll(rim, columns // 2, 1))
    normed = channel_norm(rim, *scaled(table, 4)).astype(BF)
    thirty = small_rim(total_thirty[...], normed, conv[2], columns // 2, first).astype(BF)
    own_sixteen[...] = sixteen
    own_thirty[...] = thirty
    floats = jnp.concatenate([sixteen, thirty], axis=1).astype(F32)
    sums = jnp.sum(floats, axis=0, keepdims=True)
    squares = jnp.sum(floats * floats, axis=0, keepdims=True)
    pieces = floats.shape[1] // LANES
    stats = jnp.concatenate(
        [part[:, k * LANES : (k + 1) * LANES] for part in (sums, squares) for k in range(pieces)]
        ,
        axis=0,
    )
    parts = []
    for _ in range(3):
        parts.append(stats.astype(BF))
        stats = stats - parts[-1].astype(F32)
    parts.append(jnp.zeros((out.shape[1] - NECK_ROWS - 6 * pieces, LANES), BF))
    parts = jnp.concatenate([part.astype(F32) for part in parts], axis=0).astype(BF)
    for m in range(members):
        out[m, NECK_ROWS:] = parts


def finish(band_at, got, own_sixteen, own_thirty, table, eight, sixteen, thirty, sixty):
    members = got.shape[0]
    first = band_at[0] == 0
    neck = members * NECK_ROWS
    for r in range(members):
        source = jnp.where(
            first, place(r, RETURN_ORDER), place(members - 1 - r, RETURN_ORDER)
        )
        eight[:, r * LANES : (r + 1) * LANES] = got[source, :NECK_ROWS]
    stats = jnp.sum(got[:, NECK_ROWS:].astype(F32), axis=0)
    pieces = own_sixteen.shape[1] // LANES + 1
    stats = sum(stats[2 * pieces * k : 2 * pieces * (k + 1)] for k in range(3)) / neck

    def apply(values, k, index):
        gain, shift = scaled(table, index)
        center = stats[k : k + 1]
        spread = stats[pieces + k : pieces + k + 1] - center * center
        return ((values.astype(F32) - center) * lax.rsqrt(spread + EPSILON) * gain + shift).astype(BF)

    for k in range(pieces - 1):
        at = slice(k * LANES, (k + 1) * LANES)
        sixteen[:, at] = apply(own_sixteen[:, at], k, 3)
    last = apply(own_thirty[...], pieces - 1, 5)
    thirty[...] = last
    small = LANES // 4
    pick = one_hot(
        (LANES, sixty.shape[1]),
        lambda l: (l // (small // 2)) * (2 * small) + (l % (small // 2)) * 2,
    )
    sixty[...] = dot(last, pick).astype(BF)


def call(kernel, outs, where, *operands, scratch=(), space=pltpu.VMEM):
    spaces = space if isinstance(space, tuple) else (space,) * len(operands)
    specs = [pl.BlockSpec(memory_space=pltpu.SMEM) for _ in where] + [
        pl.BlockSpec(memory_space=space) for space in spaces
    ]
    return pl.pallas_call(
        kernel,
        in_specs=specs,
        out_specs=jax.tree.map(lambda _: pl.BlockSpec(memory_space=pltpu.VMEM), outs),
        out_shape=outs,
        scratch_shapes=scratch,
        compiler_params=pltpu.CompilerParams(vmem_limit_bytes=GRANT),
    )(*where, *map(pltpu.with_memory_space_constraint, operands, spaces))


def per_device(
    features,
    deconv_weight,
    deconv_bias,
    lateral_eight,
    lateral_coarse,
    output_conv,
    norm_gain,
    norm_shift,
):
    row_count, col_count, local = features.shape
    members = lax.axis_size(MP)
    pixels = row_count * col_count
    half_local = deconv_weight.shape[1]
    neck = norm_gain.shape[1]
    assert members == MEMBERS == 2 * row_count and 2 * col_count == LANES
    assert lateral_eight.shape[0] == NECK_ROWS and members * NECK_ROWS == neck
    shape = jax.ShapeDtypeStruct
    band, row, plane = (
        lax.axis_index(axis).astype(jnp.int32).reshape(1) for axis in ("space", MP, "dp")
    )
    planes = lax.axis_size("dp")
    assert planes % SHARES == 0
    parity = plane & 1
    conv = output_conv.transpose(0, 2, 1, 3)
    share_rows = PER_SHARE * NECK_ROWS

    def from_plane(value, step):
        return lax.ppermute(value, "dp", [((i + step) % planes, i) for i in range(planes)])

    def from_core(value):
        return lax.ppermute(value, "space", [(0, 1), (1, 0)])

    bias = deconv_bias.reshape(1, half_local)
    depth = deconv_weight.shape[2]
    kept = (features, conv, lateral_eight, bias)
    sent = (deconv_weight.reshape(-1, depth), lateral_coarse.reshape(-1, depth))
    pair_rows = 4 * half_local + 3 * NECK_ROWS
    blocks, pair, pair_half = call(
        spread_features,
        (
            shape((members, local * pixels // 2 // LANES + share_rows, LANES), BF),
            shape((pair_rows, depth), BF),
            shape((pair_rows, depth // 2), BF),
        ),
        (band, parity), *kept, *sent,
        space=pltpu.HBM,
        scratch=[
            *(pltpu.VMEM(x.shape[k == 1 :], x.dtype) for k, x in enumerate(kept)),
            pltpu.SemaphoreType.DMA((len(kept) + len(sent),)),
        ],
    )
    pair_half = lax.ppermute(pair_half, MP, [(m, m ^ 1) for m in range(members)])
    gathered = exchanged(blocks, GATHER_ORDER)
    pair_other = call(
        join_halves, shape((pair_rows, depth), BF), (band,), pair_half, from_core(pair_half)
    )
    share, share_low, share_high = call(
        take_shares,
        tuple(shape((rows, share_rows, LANES), BF) for rows in (members, members // 2, members // 2)),
        (), gathered,
    )
    blocks = call(
        raise_map,
        shape((members, 3 * half_local + 5 * NECK_ROWS, LANES), BF),
        (band, row), gathered, pair, pair_other,
        scratch=[pltpu.VMEM((members, half_local, LANES), BF)],
    )
    got = exchanged(blocks, SPREAD_ORDER)
    share_low = from_plane(share_low, -1)
    share_high = from_plane(share_high, 1)
    mine = call(
        merge_shares,
        shape((SHARES, members, share_rows, LANES), BF),
        (parity,), share, share_low, share_high,
    )
    theirs = from_core(mine)
    got_other = from_core(got)
    where = (band, row)
    weights = (mine, theirs)
    total, total_sixteen, total_thirty = call(
        own_band,
        (
            shape((neck, LANES), F32),
            shape((NECK_ROWS, pixels), F32),
            shape((NECK_ROWS, pixels // 4), F32),
        ),
        where, got, *weights, conv, norm_gain, norm_shift,
    )
    blocks, own_sixteen, own_thirty, table = call(
        levels,
        (
            shape((members, 3 * NECK_ROWS, LANES), BF),
            shape((NECK_ROWS, pixels), BF),
            shape((NECK_ROWS, pixels // 4), BF),
            shape((NECK_ROWS, 16), F32),
        ),
        where, got_other, total, total_sixteen, total_thirty, *weights, conv, norm_gain, norm_shift,
        scratch=[pltpu.VMEM((neck, 16), F32)],
    )
    got = exchanged(blocks, RETURN_ORDER)
    return call(
        finish,
        (
            shape((NECK_ROWS, 4 * pixels), BF),
            shape((NECK_ROWS, pixels), BF),
            shape((NECK_ROWS, pixels // 4), BF),
            shape((NECK_ROWS, pixels // 16), BF),
        ),
        (band,), got, own_sixteen, own_thirty, table,
    )


def solution(mesh):
    finer = Mesh(
        mesh.devices.reshape(mesh.shape["dp"], mesh.shape["space"], 4, 4),
        ("dp", "space", "mp_0", "mp_1"),
    )
    in_specs = (
        P(("dp", "space"), None, MP),
        P(None, MP, None),
        P(MP),
        P(MP, None),
        P(None, MP, None),
        P(None, MP, None, None),
        P(),
        P(),
    )
    return jax.shard_map(
        per_device,
        mesh=finer,
        in_specs=in_specs,
        out_specs=(P(MP, ("dp", "space")),) * 4,
        check_vma=False,
    )
```
